32 devices in a mesh: rows: 8 (over z, x), cols: 4 (over y, core).
Axes of the slice: x: 2, y: 2, z: 4, core: 2. Of those that a mesh axis runs over, the one named last changes fastest.
Arguments:
- basis: bfloat16 [65536, 512], P('rows', 'cols'), may hold values from -6 to 6
- lower: bfloat16 [256, 256, 256], P('rows'), may hold values from -0.375 to 0.375
- diag: bfloat16 [256, 256, 256], P('rows'), may hold values from -0.375 to 0.375
- upper: bfloat16 [256, 256, 256], P('rows'), may hold values from -0.375 to 0.375
- inverse: bfloat16 [256, 256, 256], P('rows'), may hold values from -0.375 to 0.375
Outputs:
- ortho: bfloat16 [65536, 512], P('rows', 'cols')
- projected: float32 [512, 512], P(None, 'cols')
The draws below stay inside these ranges and needn't reach their ends.
All inputs are finite; a program needn't handle non-finite values.
Results may differ from the reference program's by a relative error of at most 0.0085.
Values may be sent and summed in bfloat16 or wider, within the bound.
A program may use at most 128 MiB of HBM per device.

```python
import jax
import jax.numpy as jnp
from jax import lax

BS = 256
K = 512
NB = 256
ORDER = 65536


def block_scale(stream_key, shape, shards, low, largest):
    def one(dim, shards_of):
        heights = jax.random.uniform(jax.random.fold_in(jax.random.fold_in(stream_key, 6), dim), (shards_of,), jnp.float32, low / len(shards), largest / len(shards))
        return jnp.repeat(jnp.exp(heights), shape[dim] // shards_of).reshape((-1,) + (1,) * (len(shape) - dim - 1))

    gain = one(*shards[0])
    for cut in shards[1:]:
        gain = gain * one(*cut)
    return gain


def scatter_about(key, extent, scale, reach, pieces=(), kind=jnp.bfloat16):
    array = scale * jax.random.normal(key, extent, jnp.float32)
    if pieces:
        array = array * block_scale(key, extent, pieces, -0.22, 0.18)
    return jnp.clip(array, -reach, reach).astype(kind)


def setup_inputs(seed: int = 0) -> dict:
    streams_of = jax.random.split(jax.random.key(seed), 6)
    return {
        "basis": scatter_about(streams_of[0], (ORDER, K), 1.0, 6.0, ((0, 8), (1, 4))),
        "lower": scatter_about(streams_of[1], (NB, BS, BS), BS ** -0.5, 0.375, ((0, 8),)),
        "diag": scatter_about(streams_of[2], (NB, BS, BS), BS ** -0.5, 0.375, ((0, 8),)),
        "upper": scatter_about(streams_of[3], (NB, BS, BS), BS ** -0.5, 0.375, ((0, 8),)),
        "inverse": scatter_about(streams_of[4], (NB, BS, BS), BS ** -0.5, 0.375, ((0, 8),)),
    }


def operate(field, lower, diag, upper, inverse):
    blocks = field.reshape(NB, BS, K).astype(jnp.float32)
    zero = jnp.zeros((1, BS, K), jnp.float32)
    before = jnp.concatenate([zero, blocks[:-1]], axis=0)
    after = jnp.concatenate([blocks[1:], zero], axis=0)
    mixed = jnp.einsum('bij,bjc->bic', lower.astype(jnp.float32), before)
    mixed = mixed + jnp.einsum('bij,bjc->bic', diag.astype(jnp.float32), blocks)
    mixed = mixed + jnp.einsum('bij,bjc->bic', upper.astype(jnp.float32), after)
    mixed = mixed.astype(jnp.bfloat16).astype(jnp.float32)
    result = jnp.einsum('bij,bjc->bic', inverse.astype(jnp.float32), mixed)
    return result.astype(jnp.bfloat16).reshape(NB * BS, K)

def reference(basis, lower, diag, upper, inverse):
    work = operate(basis, lower, diag, upper, inverse)
    gram = jnp.dot(work.T.astype(jnp.float32), work.astype(jnp.float32), preferred_element_type=jnp.float32)
    factor = jnp.linalg.cholesky(gram)
    identity = jnp.eye(K, dtype=jnp.float32)
    linv = lax.linalg.triangular_solve(factor, identity, left_side=True, lower=True)
    rinv = linv.T.astype(jnp.bfloat16)
    ortho = jnp.dot(work.astype(jnp.float32), rinv.astype(jnp.float32), preferred_element_type=jnp.float32).astype(jnp.bfloat16)
    image = operate(ortho, lower, diag, upper, inverse)
    projected = jnp.dot(ortho.T.astype(jnp.float32), image.astype(jnp.float32), preferred_element_type=jnp.float32)
    return (ortho, projected)
```

```python
import functools

import jax
import jax.numpy as jnp
from jax import lax
from jax.experimental import pallas as pl
from jax.experimental.pallas import tpu as pltpu
from jax.sharding import PartitionSpec as P

LANES = 128
CHUNK = 2
MESH = pl.DeviceIdType.MESH
VMEM = pl.BlockSpec(memory_space=pltpu.VMEM)
ANY = pl.BlockSpec(memory_space=pl.ANY)
SUB = 8
HI = lax.Precision.HIGHEST

def factor_tile(block):
    size = block.shape[0]
    wide = (SUB, size)
    tiles = size // SUB
    row_of = lax.broadcasted_iota(jnp.int32, wide, 0)
    lane_of = lax.broadcasted_iota(jnp.int32, wide, 1)
    a = [block[t * SUB:(t + 1) * SUB, :] for t in range(tiles)]
    m = [jnp.where(lane_of == row_of + t * SUB, 1.0, 0.0).astype(jnp.float32) for t in range(tiles)]
    out = []
    for t in range(tiles):
        at, mt = a[t], m[t]
        base = t * SUB
        pivot = {}
        for i in range(SUB):
            for j in range(i + 1):
                pivot[i, j] = jnp.broadcast_to(at[i:i + 1, base + j:base + j + 1], wide)
        ra = [jnp.broadcast_to(at[i:i + 1, :], wide) for i in range(SUB)]
        rm = [jnp.broadcast_to(mt[i:i + 1, :], wide) for i in range(SUB)]
        last = t == tiles - 1
        unit = {}
        sa, sm = [None] * SUB, [None] * SUB
        fin = jnp.zeros(wide, jnp.float32)
        for j in range(SUB):
            d = pivot[j, j]
            root = lax.rsqrt(d)
            inv = 1.0 / d
            fin = jnp.where(row_of == j, rm[j] * root, fin)
            for i in range(j + 1, SUB):
                unit[i, j] = pivot[i, j] * inv
            for i in range(j + 1, SUB):
                for q in range(j + 1, i + 1):
                    pivot[i, q] = pivot[i, q] - unit[i, j] * pivot[q, j]
            for i in range(j + 1, SUB):
                if not last:
                    ra[i] = ra[i] - unit[i, j] * ra[j]
                rm[i] = rm[i] - unit[i, j] * rm[j]
            if not last:
                sa[j] = ra[j] * inv
                sm[j] = rm[j] * inv
        out.append(fin)
        if last:
            break
        for j in range(SUB - 1, -1, -1):
            for i in range(j):
                sa[i] = sa[i] - unit[j, i] * sa[j]
                sm[i] = sm[i] - unit[j, i] * sm[j]
        for s in range(t + 1, tiles):
            na, nm = a[s], m[s]
            for j in range(SUB):
                c = jnp.broadcast_to(a[s][:, base + j:base + j + 1], wide)
                na = na - c * sa[j]
                nm = nm - c * sm[j]
            a[s], m[s] = na, nm
    return jnp.concatenate(out, axis=0)

def inverse_upper_steps(work_ref, out_ref, panel_ref):
    n, size, _ = work_ref.shape
    order = n * size
    def step(b, carry):
        at = [work_ref[b, :, i * size:(i + 1) * size] for i in range(n)]
        block = at[0]
        for i in range(1, n):
            block = jnp.where(b == i, at[i], block)
        linv = factor_tile(block)
        live = pl.ds(pl.multiple_of(b * size, size), order + size)
        work_ref[b, :, live] = lax.dot_general(
            linv, work_ref[b, :, live], (((1,), (0,)), ((), ())), precision=HI,
            preferred_element_type=jnp.float32,
        )
        for i in range(n):
            panel_ref[i] = work_ref[b, :, i * size:(i + 1) * size]

        def below(i, c):
            work_ref[i, :, live] = work_ref[i, :, live] - lax.dot_general(
                panel_ref[i], work_ref[b, :, live], (((0,), (0,)), ((), ())), precision=HI,
                preferred_element_type=jnp.float32,
            )
            return c

        lax.fori_loop(b + 1, n, below, 0)
        return carry
    lax.fori_loop(0, n, step, 0)
    for b in range(n):
        out_ref[:, b * size:(b + 1) * size] = work_ref[b, :, order:].T.astype(out_ref.dtype)

def unpack_kernel(packed_ref, out_ref, work_ref, panel_ref):
    n, size, _ = work_ref.shape
    order = n * size
    row = lax.broadcasted_iota(jnp.int32, (size, order), 0)
    lane = lax.broadcasted_iota(jnp.int32, (size, order), 1)
    place = 0
    for i in range(n):
        work_ref[i, :, :order] = jnp.zeros((size, order), jnp.float32)
        work_ref[i, :, order:] = jnp.where(lane == row + i * size, 1.0, 0.0).astype(jnp.float32)
        for j in range(i, n):
            work_ref[i, :, j * size:(j + 1) * size] = packed_ref[place * size:(place + 1) * size, :]
            place += 1
    inverse_upper_steps(work_ref, out_ref, panel_ref)


def inverse_upper(packed, order):
    n = order // LANES
    return pl.pallas_call(
        unpack_kernel,
        out_shape=jax.ShapeDtypeStruct((order, order), jnp.bfloat16),
        in_specs=[VMEM],
        out_specs=VMEM,
        scratch_shapes=[
            pltpu.VMEM((n, LANES, 2 * order), jnp.float32),
            pltpu.VMEM((n, LANES, LANES), jnp.float32),
        ],
        cost_estimate=pl.CostEstimate(
            flops=8 * order**3, bytes_accessed=8 * order * order, transcendentals=0
        ),
        name="inverse_upper",
    )(packed)


def dot(left, right):
    return jnp.dot(left, right, preferred_element_type=jnp.float32)


def inner(left, right):
    return lax.dot_general(
        left, right, (((0,), (0,)), ((), ())), preferred_element_type=jnp.float32
    )


def remote(src, dst, send, recv, **where):
    return pltpu.make_async_remote_copy(
        src_ref=src, dst_ref=dst, send_sem=send, recv_sem=recv, device_id=where, device_id_type=MESH
    )


def exchange(axis, count, me, source, target, arrived, send, recv):
    for step in range(1, count):
        peer = lax.rem(me + step, count)
        remote(source(peer), target(me), send.at[step], recv.at[me], **{axis: peer}).start()

    def finish():
        for step in range(1, count):
            peer = lax.rem(me + step, count)
            remote(
                source(peer), arrived(peer), send.at[step], recv.at[peer], **{axis: peer}
            ).wait()

    return finish


def flip(index, bit):
    return index + bit - 2 * bit * lax.rem(index // bit, 2)


def flips(index, mask):
    bit = 1
    while bit <= mask:
        if mask & bit:
            index = flip(index, bit)
        bit *= 2
    return index


def apply_block(i, size, field, wl, wd, wu, wi):
    def at(k):
        return field[pl.ds(pl.multiple_of(k * size, size), size), :]

    mixed = dot(wl[i], at(i)) + dot(wd[i], at(i + 1)) + dot(wu[i], at(i + 2))
    return dot(wi[i], mixed.astype(jnp.bfloat16)).astype(jnp.bfloat16)


def fetch_blocks(parts, held, sem, first):
    count = held[0].shape[0]
    copies = [
        pltpu.make_async_copy(part.at[pl.ds(first * count, count)], ref, sem.at[k])
        for k, (part, ref) in enumerate(zip(parts, held))
    ]
    for copy in copies:
        copy.start()
    return copies


def greet(nr, nc, r, c):
    barrier = pltpu.get_barrier_semaphore()

    def hello(**where):
        pl.semaphore_signal(barrier, inc=1, device_id=where, device_id_type=MESH)

    for step in range(1, nc):
        hello(cols=lax.rem(c + step, nc))
    for step in range(1, nr):
        hello(rows=lax.rem(r + step, nr))
    for k in range(nc):
        pl.when((c == 0) & (r > 0) & (k != c))(lambda: hello(rows=r - 1, cols=k))
        pl.when((c == nc - 1) & (r < nr - 1) & (k != c))(lambda: hello(rows=r + 1, cols=k))
    below = ((r < nr - 1) & (c != 0)).astype(jnp.int32)
    above = ((r > 0) & (c != nc - 1)).astype(jnp.int32)
    pl.semaphore_wait(barrier, nc + nr - 2 + below + above)


def front_kernel(
    nr, nc, basis, lower, diag, upper, inverse, wext, gram,
    field, wl, wd, wu, wi, total, packed, got1, part, got2,
    wsem, lsem, fsend, frecv, hsend, hrecv, s1, r1, s2, r2, s3, r3, s4, r4,
):
    r, c = lax.axis_index("rows"), lax.axis_index("cols")
    count, size, _ = wl.shape
    width = basis.shape[1]
    body = count * size
    top = (count + 1) * size
    share = got1.shape[1]
    piece = got2.shape[1]

    weights = fetch_blocks((lower, diag, upper, inverse), (wl, wd, wu, wi), wsem, c)
    greet(nr, nc, r, c)

    def columns(k):
        return pl.ds(pl.multiple_of(k * width, width), width)

    def rows(start, extent):
        return pl.ds(pl.multiple_of(start, size), extent)

    group = CHUNK * size
    lump = body // group
    high = lump + 1
    spans = [(0, size)] + [(size + k * group, group) for k in range(lump)] + [(top, size)]

    def landing(kind, k):
        start, extent = spans[kind]
        return field.at[pl.ds(start, extent), columns(k)]

    def leaving(kind, d):
        start, extent = spans[kind]
        return basis.at[rows(d * body - size + start, extent), :]

    def to_peer(step, kind):
        d = lax.rem(c + step, nc)
        return remote(leaving(kind, d), landing(kind, c), fsend.at[kind, step], frecv.at[kind, c], cols=d)

    def own(kind):
        return pltpu.make_async_copy(leaving(kind, c), landing(kind, c), lsem.at[kind])

    def down():
        return remote(
            basis.at[pl.ds(nc * body - size, size), :], landing(0, c), fsend.at[0, 0], frecv.at[0, c],
            rows=r + 1, cols=0,
        )

    def up():
        return remote(
            basis.at[pl.ds(0, size), :], landing(high, c), fsend.at[high, 0], frecv.at[high, c],
            rows=r - 1, cols=nc - 1,
        )

    def each(kind, action):
        for step in range(1, nc):
            d = lax.rem(c + step, nc)
            send = functools.partial(action, step, kind)
            if kind == 0:
                pl.when(d > 0)(send)
            elif kind == high:
                pl.when(d < nc - 1)(send)
            else:
                send()

    def mine_too(kind, action):
        if kind == 0:
            pl.when(c > 0)(action)
        elif kind == high:
            pl.when(c < nc - 1)(action)
        else:
            action()

    pl.when(r < nr - 1)(lambda: down().start())
    for kind in range(high + 1):
        mine_too(kind, lambda: own(kind).start())
        each(kind, lambda step, kind: to_peer(step, kind).start())
        if kind == 1:
            pl.when(r > 0)(lambda: up().start())

    @pl.when((r == 0) & (c == 0))
    def _():
        field[0:size, :] = jnp.zeros((size, field.shape[1]), field.dtype)
        wext[0:size, :] = jnp.zeros((size, field.shape[1]), field.dtype)

    @pl.when((r == nr - 1) & (c == nc - 1))
    def _():
        field[top:top + size, :] = jnp.zeros((size, field.shape[1]), field.dtype)
        wext[top:top + size, :] = jnp.zeros((size, field.shape[1]), field.dtype)

    total[...] = jnp.zeros_like(total)

    def arrive(kind, k):
        start, extent = spans[kind]
        remote(
            basis.at[pl.ds(0, extent), :], landing(kind, k), fsend.at[kind, 0], frecv.at[kind, k], cols=k
        ).wait_recv()

    def block(i, carry):
        w = apply_block(i, size, field, wl, wd, wu, wi)
        wext[rows((i + 1) * size, size), :] = w
        total[...] += inner(w, w)
        return carry

    for copy in weights:
        copy.wait()
    done = 0
    for kind in range(high + 1):
        mine_too(kind, lambda: own(kind).wait())
        for k in range(nc):
            comes = k != c
            if kind == 0:
                comes = ((c > 0) & comes) | ((c == 0) & (r > 0))
            elif kind == high:
                comes = ((c < nc - 1) & comes) | ((c == nc - 1) & (r < nr - 1))
            pl.when(comes)(lambda: arrive(kind, k))
        ready = count if kind == high else max(kind * CHUNK - 1, 0)
        if ready > done:
            lax.fori_loop(done, ready, block, 0)
            done = ready

    flat = r * nc + c
    last = nr * nc - 1

    def halo(kind):
        start = (body, size)[kind]
        target = (0, top)[kind]
        to = flat + (1, -1)[kind]
        return remote(
            wext.at[pl.ds(start, size), :], wext.at[pl.ds(target, size), :], hsend.at[kind], hrecv.at[kind],
            rows=to // nc, cols=lax.rem(to, nc),
        )

    place = 0
    across = total.shape[0] // LANES
    for i in range(across):
        for j in range(i, across):
            packed[place * LANES:(place + 1) * LANES, :] = total[
                i * LANES:(i + 1) * LANES, j * LANES:(j + 1) * LANES
            ]
            place += 1
    spare = packed.shape[0] - place * LANES
    if spare:
        packed[place * LANES:, :] = jnp.zeros((spare, LANES), jnp.float32)

    def tile(ref, start, extent):
        return ref.at[pl.ds(pl.multiple_of(start, 8), extent), :]

    finish = exchange(
        "cols", nc, c, lambda d: tile(packed, d * share, share), lambda k: got1.at[k],
        lambda k: got1.at[k], s1, r1,
    )
    got1[c] = packed[pl.ds(pl.multiple_of(c * share, 8), share), :]
    finish()
    pl.when(flat < last)(lambda: halo(0).start())
    pl.when(flat > 0)(lambda: halo(1).start())
    part[...] = sum((got1[k] for k in range(1, nc)), got1[0])
    finish = exchange(
        "rows", nr, r, lambda d: tile(part, d * piece, piece), lambda k: got2.at[k],
        lambda k: got2.at[k], s2, r2,
    )
    got2[r] = part[pl.ds(pl.multiple_of(r * piece, 8), piece), :]
    finish()
    mine = c * share + r * piece
    gram[pl.ds(pl.multiple_of(mine, 8), piece), :] = sum((got2[k] for k in range(1, nr)), got2[0])
    exchange(
        "rows", nr, r, lambda d: tile(gram, mine, piece), lambda k: tile(gram, mine, piece),
        lambda k: tile(gram, c * share + k * piece, piece), s3, r3,
    )()
    exchange(
        "cols", nc, c, lambda d: tile(gram, c * share, share), lambda k: tile(gram, c * share, share),
        lambda k: tile(gram, k * share, share), s4, r4,
    )()

    pl.when(flat < last)(lambda: halo(0).wait_send())
    pl.when(flat > 0)(lambda: halo(1).wait_send())
    pl.when(flat > 0)(lambda: halo(0).wait_recv())
    pl.when(flat < last)(lambda: halo(1).wait_recv())
    pl.when(r < nr - 1)(lambda: down().wait_send())
    pl.when(r > 0)(lambda: up().wait_send())
    for kind in range(high + 1):
        each(kind, lambda step, kind: to_peer(step, kind).wait_send())


def back_kernel(
    nr, nc, wext, rinv, ortho, projected,
    oext, wl, wd, wu, wi, total, got1, part, got2,
    lsem, osend, orecv, esend, erecv, s1, r1, s2, r2, s3, r3,
):
    r, c = lax.axis_index("rows"), lax.axis_index("cols")
    count, size, _ = wl.shape
    width = ortho.shape[1]
    body = count * size
    piece = got2.shape[1]

    def at(i):
        return pl.ds(pl.multiple_of(i * size, size), size)

    def turn(i, carry):
        oext[at(i), :] = dot(wext[at(i), :], rinv[...]).astype(jnp.bfloat16)
        return carry

    lax.fori_loop(0, count // 2 + 1, turn, 0)

    early = (count // 2) * size

    def columns(start, extent, k):
        return oext.at[pl.ds(size + start, extent), pl.ds(pl.multiple_of(k * width, width), width)]

    def home(start, extent, k):
        return ortho.at[pl.ds(pl.multiple_of(k * body + start, size), extent), :]

    def go_home(start, extent, send, recv):
        there = functools.partial(home, start, extent)
        return exchange(
            "cols", nc, c, functools.partial(columns, start, extent), there, there, send, recv
        )

    finish_early = go_home(0, early, osend, orecv)
    lax.fori_loop(count // 2 + 1, count + 2, turn, 0)
    own = pltpu.make_async_copy(columns(0, body, c), home(0, body, c), lsem)
    own.start()
    total[...] = jnp.zeros_like(total)

    def block(i, carry):
        image = apply_block(i, size, oext, wl, wd, wu, wi)
        total[...] += inner(oext[at(i + 1), :], image)
        return carry

    lax.fori_loop(0, count, block, 0)

    def slab(k):
        return pl.ds(pl.multiple_of(k * width, width), width)

    bit, used = 1, 0
    kept = list(range(0, nc))
    while bit < nc:
        peer = flip(c, bit)
        kept = [k for k in kept if k & bit == 0]
        copies = [
            remote(
                total.at[:, slab(flips(peer, k))], got1.at[used + n], s1.at[used + n], r1.at[used + n],
                cols=peer,
            )
            for n, k in enumerate(kept)
        ]
        for copy in copies:
            copy.start()
        if 2 * bit == nc:
            finish_late = go_home(early, body - early, esend, erecv)
        for n, (k, copy) in enumerate(zip(kept, copies)):
            copy.wait()
            where = slab(flips(c, k))
            if 2 * bit == nc:
                part[...] = total[:, where] + got1[used + n]
            else:
                total[:, where] = total[:, where] + got1[used + n]
        used += len(kept)
        bit *= 2

    def tile(ref, k):
        return ref.at[pl.ds(pl.multiple_of(k * piece, 8), piece), :]

    finish = exchange(
        "rows", nr, r, lambda d: tile(part, d), lambda k: got2.at[k], lambda k: got2.at[k], s2, r2
    )
    got2[r] = part[pl.ds(pl.multiple_of(r * piece, 8), piece), :]
    finish()
    projected[pl.ds(pl.multiple_of(r * piece, 8), piece), :] = sum(
        (got2[k] for k in range(1, nr)), got2[0]
    )
    exchange(
        "rows", nr, r, lambda d: tile(projected, r), lambda k: tile(projected, r),
        lambda k: tile(projected, k), s3, r3,
    )()
    own.wait()
    finish_early()
    finish_late()


def whole_kernel(
    nr, nc, basis, lower, diag, upper, inverse, ortho, projected,
    field, wext, gram, rinv, wl, wd, wu, wi, total, packed, got1, part, got2, cwork, cpanel, pgot1, ppart, pgot2, *sems
):
    front, back = sems[:14], sems[14:]
    front_kernel(
        nr, nc, basis, lower, diag, upper, inverse, wext, gram,
        field, wl, wd, wu, wi, total, packed, got1, part, got2, *front,
    )
    unpack_kernel(gram, rinv, cwork, cpanel)
    back_kernel(nr, nc, wext, rinv, ortho, projected, field, wl, wd, wu, wi, total, pgot1, ppart, pgot2, *back)


def shards(nr, nc, basis, lower, diag, upper, inverse):
    blocks, size, _ = diag.shape
    width = basis.shape[1]
    order = width * nc
    count = blocks // nc
    across = order // LANES
    tiles = across * (across + 1) // 2 * LANES // 8
    piece = -(-tiles // (nr * nc)) * 8
    share = piece * nr
    dma = pltpu.SemaphoreType.DMA
    held = [pltpu.VMEM((count, size, size), jnp.bfloat16)] * 4
    extended = ((count + 2) * size, order)
    pair = lambda n: [dma((n,)), dma((n,))]
    kinds = count // CHUNK + 2
    lines = order // nr
    f32 = jnp.float32
    return pl.pallas_call(
        functools.partial(whole_kernel, nr, nc),
        out_shape=(
            jax.ShapeDtypeStruct(basis.shape, jnp.bfloat16),
            jax.ShapeDtypeStruct((order, width), f32),
        ),
        in_specs=[ANY] * 5,
        out_specs=(ANY, VMEM),
        scratch_shapes=[
            pltpu.VMEM(extended, jnp.bfloat16),
            pltpu.VMEM(extended, jnp.bfloat16),
            pltpu.VMEM((nc * share, LANES), f32),
            pltpu.VMEM((order, order), jnp.bfloat16),
        ] + held + [
            pltpu.VMEM((order, order), f32),
            pltpu.VMEM((nc * share, LANES), f32),
            pltpu.VMEM((nc, share, LANES), f32),
            pltpu.VMEM((share, LANES), f32),
            pltpu.VMEM((nr, piece, LANES), f32),
            pltpu.VMEM((across, LANES, 2 * order), f32),
            pltpu.VMEM((across, LANES, LANES), f32),
            pltpu.VMEM((nc, order, width), f32),
            pltpu.VMEM((order, width), f32),
            pltpu.VMEM((nr, lines, width), f32),
            dma((4,)), dma((kinds,)), dma((kinds, nc)), dma((kinds, nc)), dma((2,)), dma((2,)),
        ] + pair(nc) + pair(nr) + pair(nr) + pair(nc)
        + [dma] + pair(nc) + pair(nc) + pair(nc) + pair(nr) + pair(nr),
        compiler_params=pltpu.CompilerParams(has_side_effects=True, collective_id=1),
        name="krylov",
    )(basis, lower, diag, upper, inverse)


def solution(mesh):
    in_specs = (
        P("rows", "cols"),
        P("rows", None, None),
        P("rows", None, None),
        P("rows", None, None),
        P("rows", None, None),
    )
    out_specs = (P("rows", "cols"), P(None, "cols"))
    body = functools.partial(shards, mesh.shape["rows"], mesh.shape["cols"])
    return jax.shard_map(body, mesh=mesh, in_specs=in_specs, out_specs=out_specs, check_vma=False)
```

```python
import functools

import jax
import jax.numpy as jnp
from jax import lax
from jax.experimental import pallas as pl
from jax.experimental.pallas import tpu as pltpu
from jax.sharding import PartitionSpec as P

LANES = 128
MESH = pl.DeviceIdType.MESH
VMEM = pl.BlockSpec(memory_space=pltpu.VMEM)
ANY = pl.BlockSpec(memory_space=pl.ANY)
SUB = 8
HI = lax.Precision.HIGHEST

def factor_tile(block):
    size = block.shape[0]
    wide = (SUB, size)
    tiles = size // SUB
    row_of = lax.broadcasted_iota(jnp.int32, wide, 0)
    lane_of = lax.broadcasted_iota(jnp.int32, wide, 1)
    a = [block[t * SUB:(t + 1) * SUB, :] for t in range(tiles)]
    out = []
    for t in range(tiles):
        base = t * SUB
        at = a[t]
        inside = (lane_of >= base) & (lane_of < base + SUB)
        unity = jnp.where(lane_of == row_of + base, 1.0, 0.0).astype(jnp.float32)
        mixed = jnp.where(inside, unity, at)
        pivot = {}
        for i in range(SUB):
            for j in range(i + 1):
                pivot[i, j] = jnp.broadcast_to(at[i:i + 1, base + j:base + j + 1], wide)
        rows = [jnp.broadcast_to(mixed[i:i + 1, :], wide) for i in range(SUB)]
        last = t == tiles - 1
        unit = {}
        solved = [None] * SUB
        fin = jnp.zeros(wide, jnp.float32)
        for j in range(SUB):
            d = pivot[j, j]
            root = lax.rsqrt(d)
            inv = 1.0 / d
            fin = jnp.where(row_of == j, rows[j] * root, fin)
            for i in range(j + 1, SUB):
                unit[i, j] = pivot[i, j] * inv
            for i in range(j + 1, SUB):
                for q in range(j + 1, i + 1):
                    pivot[i, q] = pivot[i, q] - unit[i, j] * pivot[q, j]
            for i in range(j + 1, SUB):
                rows[i] = rows[i] - unit[i, j] * rows[j]
            if not last:
                solved[j] = rows[j] * inv
        out.append(jnp.where(lane_of < base + SUB, fin, 0.0))
        if last:
            break
        for j in range(SUB - 1, -1, -1):
            for i in range(j):
                solved[i] = solved[i] - unit[j, i] * solved[j]
        for s in range(t + 1, tiles):
            new = jnp.where(inside, 0.0, a[s])
            for j in range(SUB - 1, -1, -1):
                c = jnp.broadcast_to(a[s][:, base + j:base + j + 1], wide)
                new = new - c * solved[j]
            a[s] = new
    return jnp.concatenate(out, axis=0)


def inverse_lower(work_ref, out_ref, panel_ref):
    n, size, _ = work_ref.shape
    order = n * size

    def step(b, carry):
        at = [work_ref[b, :, i * size:(i + 1) * size] for i in range(n)]
        block = at[0]
        for i in range(1, n):
            block = jnp.where(b == i, at[i], block)
        linv = factor_tile(block)
        live = pl.ds(pl.multiple_of(b * size, size), order + size)
        work_ref[b, :, live] = lax.dot_general(
            linv, work_ref[b, :, live], (((1,), (0,)), ((), ())), precision=HI,
            preferred_element_type=jnp.float32,
        )
        for i in range(n):
            panel_ref[i] = work_ref[b, :, i * size:(i + 1) * size]

        def below(i, c):
            work_ref[i, :, live] = work_ref[i, :, live] - lax.dot_general(
                panel_ref[i], work_ref[b, :, live], (((0,), (0,)), ((), ())), precision=HI,
                preferred_element_type=jnp.float32,
            )
            return c

        lax.fori_loop(b + 1, n, below, 0)
        return carry

    lax.fori_loop(0, n, step, 0)
    for b in range(n):
        out_ref[b * size:(b + 1) * size, :] = work_ref[b, :, order:]


def augment(work_ref):
    n, size, _ = work_ref.shape
    order = n * size
    row = lax.broadcasted_iota(jnp.int32, (size, order), 0)
    lane = lax.broadcasted_iota(jnp.int32, (size, order), 1)
    for i in range(n):
        work_ref[i, :, :order] = jnp.zeros((size, order), jnp.float32)
        work_ref[i, :, order:] = jnp.where(lane == row + i * size, 1.0, 0.0).astype(jnp.float32)


def dot(left, right):
    return jnp.dot(left, right, preferred_element_type=jnp.float32)


def inner(left, right):
    return lax.dot_general(
        left, right, (((0,), (0,)), ((), ())), preferred_element_type=jnp.float32
    )


def fine(left, right, dims=((1,), (0,))):
    return lax.dot_general(
        left, right, (dims, ((), ())), precision=HI, preferred_element_type=jnp.float32
    )


def remote(src, dst, send, recv, **where):
    return pltpu.make_async_remote_copy(
        src_ref=src, dst_ref=dst, send_sem=send, recv_sem=recv, device_id=where, device_id_type=MESH
    )


def exchange(count, me, where, source, target, arrived, send, recv):
    for step in range(1, count):
        peer = lax.rem(me + step, count)
        remote(source(peer), target(me), send.at[step], recv.at[me], **where(peer)).start()

    def finish():
        for step in range(1, count):
            peer = lax.rem(me + step, count)
            remote(
                source(peer), arrived(peer), send.at[step], recv.at[peer], **where(peer)
            ).wait()

    return finish


def greet(nr, nc, r, c):
    barrier = pltpu.get_barrier_semaphore()
    flat = r * nc + c
    total = nr * nc

    def hello(step, carry):
        to = lax.rem(flat + step, total)
        pl.semaphore_signal(
            barrier, inc=1, device_id=dict(rows=to // nc, cols=lax.rem(to, nc)), device_id_type=MESH
        )
        return carry

    lax.fori_loop(1, total, hello, 0)
    pl.semaphore_wait(barrier, total - 1)


def lined(ref, start, extent):
    return ref.at[pl.ds(pl.multiple_of(start, 8), extent), :]


def summed(ref, count):
    return sum((ref[k] for k in range(1, count)), ref[0])


def whole_kernel(
    nr, nc, basis, lower, diag, upper, inverse, ortho, projected,
    bext, wext, wsend, oext, wl, wd, wu, wi, gy, gx, total, rinv, cwork, cpanel, linv0, linv1, tall,
    ypack, ygot1, ypart, ygot2, yall, xpack, xgot1, xpart, xgot2, xall,
    pmine, pgot1, phalf, pgot2, psum, ppack, pgot3, pall,
    wsem, lsem, bsend, brecv, esem, osem, orecv, hsend, hrecv, isem, *sems,
):
    sems = list(sems)

    def pair():
        return sems.pop(0), sems.pop(0)

    bf16, f32 = jnp.bfloat16, jnp.float32
    r, c = lax.axis_index("rows"), lax.axis_index("cols")
    h = nc // 2
    y, p = c // h, lax.rem(c, h)
    other = (1 - y) * h + p
    _, count, size, _ = wl.shape
    width = basis.shape[1]
    half = width * h
    order = 2 * half
    body = count * size
    bottom = size + body
    team = 2 * nr
    seat = 2 * r + y

    def mate(k):
        return dict(cols=y * h + k)

    def member(k):
        return dict(rows=k // 2, cols=lax.rem(k, 2) * h + p)

    def line(k):
        return dict(rows=k)

    def at(i):
        return pl.ds(pl.multiple_of(i * size, size), size)

    def lanes(k, extent):
        return pl.ds(pl.multiple_of(k * extent, LANES), extent)

    weights = []
    for j, g in enumerate((other, c)):
        batch = [
            pltpu.make_async_copy(part.at[pl.ds(g * count, count)], held.at[j], wsem.at[j, k])
            for k, (part, held) in enumerate(zip((lower, diag, upper, inverse), (wl, wd, wu, wi)))
        ]
        for copy in batch:
            copy.start()
        weights.append(batch)

    spans = [(0, size), (size, body), (bottom, size)]

    def group(j, k):
        return y * h + k if j else (1 - y) * h + k

    def leaving(j, s, k):
        start, extent = spans[s]
        return basis.at[pl.ds(pl.multiple_of(group(j, k) * body - size + start, size), extent), :]

    def landing(j, s, k):
        start, extent = spans[s]
        return bext.at[j, pl.ds(start, extent), lanes(k, width)]

    def within(s, g, action):
        if s == 0:
            pl.when(g > 0)(action)
        elif s == 2:
            pl.when(g < nc - 1)(action)
        else:
            action()

    def own(j, s):
        return pltpu.make_async_copy(leaving(j, s, p), landing(j, s, p), lsem.at[j, s])

    def to_mate(j, s, step):
        k = lax.rem(p + step, h)
        return remote(leaving(j, s, k), landing(j, s, p), bsend.at[j, s, step], brecv.at[j, s, p], **mate(k))

    def down():
        return remote(
            basis.at[pl.ds(nc * body - size, size), :], landing(1 - y, 0, p), esem.at[0],
            brecv.at[1 - y, 0, p], rows=r + 1, cols=y * h,
        )

    def up():
        return remote(
            basis.at[pl.ds(0, size), :], landing(y, 2, p), esem.at[1],
            brecv.at[y, 2, p], rows=r - 1, cols=y * h + h - 1,
        )

    for j in (0, 1):
        for s in (1, 0, 2):
            within(s, group(j, p), lambda: own(j, s).start())

    greet(nr, nc, r, c)

    def each(j, s, action):
        for step in range(1, h):
            k = lax.rem(p + step, h)
            within(s, group(j, k), functools.partial(action, step))

    for step in range(1, h):
        to_mate(0, 1, step).start()
    pl.when(r < nr - 1)(lambda: down().start())
    pl.when(r > 0)(lambda: up().start())
    for j, s in ((0, 0), (0, 2), (1, 1), (1, 0), (1, 2)):
        each(j, s, lambda step: to_mate(j, s, step).start())

    for j in (0, 1):
        @pl.when((r == 0) & (group(j, p) == 0))
        def _():
            bext[j, 0:size, :] = jnp.zeros((size, half), bf16)

        @pl.when((r == nr - 1) & (group(j, p) == nc - 1))
        def _():
            bext[j, bottom:bottom + size, :] = jnp.zeros((size, half), bf16)

    @pl.when((r == 0) & (c == 0))
    def _():
        wext[0:size, :] = jnp.zeros((size, order), bf16)

    @pl.when((r == nr - 1) & (c == nc - 1))
    def _():
        wext[bottom:bottom + size, :] = jnp.zeros((size, order), bf16)

    def arrive(j, s):
        g = group(j, p)
        within(s, g, lambda: own(j, s).wait())
        for k in range(h):
            comes = k != p
            if s == 0:
                comes = ((g > 0) & comes) | ((g == 0) & (r > 0))
            elif s == 2:
                comes = ((g < nc - 1) & comes) | ((g == nc - 1) & (r < nr - 1))
            extent = spans[s][1]
            pl.when(comes)(
                lambda: remote(
                    basis.at[pl.ds(0, extent), :], landing(j, s, k), bsend.at[j, s, 0], brecv.at[j, s, k], **mate(k)
                ).wait_recv()
            )

    def applied(field, j, i, columns):
        mixed = (
            dot(wl[j, i], field[i * size:(i + 1) * size, columns])
            + dot(wd[j, i], field[(i + 1) * size:(i + 2) * size, columns])
            + dot(wu[j, i], field[(i + 2) * size:(i + 3) * size, columns])
        )
        return dot(wi[j, i], mixed.astype(bf16)).astype(bf16)

    mine = lanes(y, half)
    chunks = [(i, 2) for i in range(1, count - 1, 2)] + [(0, 1), (count - 1, 1)]

    def cross(n, to=None):
        start, extent = chunks[n][0] * size, chunks[n][1] * size
        return remote(
            wsend.at[pl.ds(start, extent), :],
            wext.at[pl.ds(size + start, extent), mine if to is None else to],
            osem.at[n], orecv.at[n], cols=other,
        )

    gy[...] = jnp.zeros_like(gy)
    for copy in weights[0]:
        copy.wait()
    arrive(0, 1)
    held_back = max(len(chunks) - 3, 1)
    for n, (first, extent) in enumerate(chunks):
        if first == 0:
            arrive(0, 0)
            arrive(0, 2)
        ws = []
        for i in range(first, first + extent):
            w = applied(bext.at[0], 0, i, slice(None))
            wsend[i * size:(i + 1) * size, :] = w
            ws.append(w)
        if n < held_back:
            cross(n).start()
        gy[...] += sum(inner(w, w) for w in ws)
    for copy in weights[1]:
        copy.wait()
    arrive(1, 1)
    for n, (first, extent) in enumerate(chunks):
        if first == 0:
            arrive(1, 0)
            arrive(1, 2)
        ws = []
        for i in range(first, first + extent):
            w = applied(bext.at[1], 1, i, slice(None))
            wext[(i + 1) * size:(i + 2) * size, mine] = w
            ws.append(w)
        gy[...] += sum(inner(w, w) for w in ws)

    across = half // LANES
    place = 0
    for i in range(across):
        for j in range(i, across):
            ypack[place * LANES:(place + 1) * LANES, :] = gy[
                i * LANES:(i + 1) * LANES, j * LANES:(j + 1) * LANES
            ]
            place += 1
    if ypack.shape[0] > place * LANES:
        ypack[place * LANES:, :] = jnp.zeros((ypack.shape[0] - place * LANES, LANES), f32)
    share, piece = ygot1.shape[1], ygot2.shape[1]
    s, v = pair()
    finish = exchange(
        h, p, mate, lambda d: lined(ypack, d * share, share), lambda k: ygot1.at[k], lambda k: ygot1.at[k], s, v
    )
    ygot1[p] = ypack[pl.ds(pl.multiple_of(p * share, 8), share), :]
    finish()
    ypart[...] = summed(ygot1, h)
    s, v = pair()
    finish = exchange(
        nr, r, line, lambda d: lined(ypart, d * piece, piece), lambda k: ygot2.at[k], lambda k: ygot2.at[k], s, v
    )
    ygot2[r] = ypart[pl.ds(pl.multiple_of(r * piece, 8), piece), :]
    finish()
    def yspot(k):
        return yall.at[lax.rem(k, 2), pl.ds(pl.multiple_of(p * share + (k // 2) * piece, 8), piece), :]
    yall[y, pl.ds(pl.multiple_of(p * share + r * piece, 8), piece), :] = summed(ygot2, nr)
    s, v = pair()
    finish = exchange(team, seat, member, lambda d: yspot(seat), lambda k: yspot(seat), yspot, s, v)
    for n in range(held_back, len(chunks)):
        cross(n).start()
    finish()
    def yshare(k):
        return yall.at[:, pl.ds(pl.multiple_of(k * share, 8), share), :]
    s, v = pair()
    exchange(h, p, mate, lambda d: yshare(p), lambda k: yshare(p), yshare, s, v)()

    def load(which):
        place = 0
        for i in range(across):
            for j in range(i, across):
                cwork[i, :, j * LANES:(j + 1) * LANES] = yall[which, place * LANES:(place + 1) * LANES, :]
                place += 1

    augment(cwork)
    load(0)
    inverse_lower(cwork, linv0, cpanel)

    gx[...] = jnp.zeros_like(gx)
    theirs = lanes(1 - y, half)
    for n, (first, extent) in enumerate(chunks):
        cross(n, theirs).wait_recv()
        rows = slice((first + 1) * size, (first + 1 + extent) * size)
        gx[...] += inner(wext[rows, :half], wext[rows, half:])

    for j in range(across):
        xpack[j * half:(j + 1) * half, :] = gx[:, j * LANES:(j + 1) * LANES]
    if xpack.shape[0] > across * half:
        xpack[across * half:, :] = jnp.zeros((xpack.shape[0] - across * half, LANES), f32)
    xshare, xpiece = xgot1.shape[1], xgot2.shape[1]
    s, v = pair()
    finish = exchange(
        h, p, mate, lambda d: lined(xpack, d * xshare, xshare), lambda k: xgot1.at[k], lambda k: xgot1.at[k], s, v
    )
    xgot1[p] = xpack[pl.ds(pl.multiple_of(p * xshare, 8), xshare), :]
    finish()
    xpart[...] = summed(xgot1, h)
    s, v = pair()
    finish = exchange(
        team, seat, member, lambda d: lined(xpart, d * xpiece, xpiece), lambda k: xgot2.at[k],
        lambda k: xgot2.at[k], s, v,
    )
    xgot2[seat] = xpart[pl.ds(pl.multiple_of(seat * xpiece, 8), xpiece), :]
    finish()
    def xspot(k):
        return lined(xall, p * xshare + k * xpiece, xpiece)
    xall[pl.ds(pl.multiple_of(p * xshare + seat * xpiece, 8), xpiece), :] = summed(xgot2, team)
    s, v = pair()
    exchange(team, seat, member, lambda d: xspot(seat), lambda k: xspot(seat), xspot, s, v)()

    flat = r * nc + c
    last = nr * nc - 1

    def halo(kind):
        start = (body, size)[kind]
        target = (0, bottom)[kind]
        to = flat + (1, -1)[kind]
        return remote(
            wext.at[pl.ds(start, size), :], wext.at[pl.ds(target, size), :], hsend.at[kind], hrecv.at[kind],
            rows=to // nc, cols=lax.rem(to, nc),
        )

    pl.when(flat < last)(lambda: halo(0).start())
    pl.when(flat > 0)(lambda: halo(1).start())
    def xsection(k):
        return lined(xall, k * xshare, xshare)
    s, v = pair()
    exchange(h, p, mate, lambda d: xsection(p), lambda k: xsection(p), xsection, s, v)()

    for j in range(across):
        gx[:, j * LANES:(j + 1) * LANES] = xall[j * half:(j + 1) * half, :]
    tall[...] = fine(linv0[...], gx[...])
    augment(cwork)
    load(1)
    for i in range(across):
        cwork[i, :, :half] = cwork[i, :, :half] - fine(
            tall[:, i * LANES:(i + 1) * LANES], tall[...], ((0,), (0,))
        )
    gx[...] = fine(tall[...], linv0[...], ((0,), (0,)))
    inverse_lower(cwork, linv1, cpanel)
    rinv[:half, :half] = linv0[...].T.astype(bf16)
    rinv[half:, half:] = linv1[...].T.astype(bf16)
    rinv[:half, half:] = (-fine(linv1[...], gx[...])).T.astype(bf16)

    def turn(i):
        oext[at(i), :half] = dot(wext[at(i), :half], rinv[:half, :half]).astype(bf16)
        oext[at(i), half:] = dot(wext[at(i), :], rinv[:, half:]).astype(bf16)

    def columns(start, extent, k):
        return oext.at[pl.ds(size + start, extent), lanes(k, width)]

    def home(start, extent, k):
        return ortho.at[pl.ds(pl.multiple_of(k * body + start, size), extent), :]

    def row(k):
        return dict(cols=k)

    def go_home(start, extent, send, recv):
        there = functools.partial(home, start, extent)
        return exchange(nc, c, row, functools.partial(columns, start, extent), there, there, send, recv)

    early = (count // 4) * size
    for i in range(1, count // 4 + 1):
        turn(i)
    s, v = pair()
    finish_early = go_home(0, early, s, v)

    def later(i, carry):
        turn(i)
        return carry

    lax.fori_loop(count // 4 + 1, count + 1, later, 0)
    placed = pltpu.make_async_copy(columns(0, body, c), home(0, body, c), isem)
    placed.start()
    pl.when(flat > 0)(lambda: halo(0).wait_recv())
    turn(0)
    pl.when(flat < last)(lambda: halo(1).wait_recv())
    turn(count + 1)
    total[...] = jnp.zeros_like(total)

    def image(i, carry):
        mixed = dot(wl[1, i], oext[at(i), :]) + dot(wd[1, i], oext[at(i + 1), :]) + dot(wu[1, i], oext[at(i + 2), :])
        z = dot(wi[1, i], mixed.astype(bf16)).astype(bf16)
        total[...] += inner(oext[at(i + 1), :], z)
        return carry

    lax.fori_loop(0, count, image, 0, unroll=2)

    n = order
    for k in range(2):
        for q in range(h):
            ppack[k, q] = total[:, (k * h + q) * width:(k * h + q + 1) * width].astype(bf16)
    s, v = pair()
    exchange(
        h, p, mate, lambda d: ppack.at[:, d], lambda k: pgot1.at[k], lambda k: pgot1.at[k], s, v
    )()
    for k in range(2):
        pmine[k] = total[:, lanes(k * h + p, width)]
    for step in range(1, h):
        for k in range(2):
            pmine[k] = pmine[k] + pgot1[lax.rem(p + step, h), k].astype(f32)
    phalf[0] = pmine[1 - y].astype(bf16)
    s, v = pair()
    crossing = remote(phalf.at[0], phalf.at[1], s.at[0], v.at[0], cols=other)
    crossing.start()
    s, v = pair()
    finish_late = go_home(early, body - early, s, v)
    crossing.wait()
    psum[...] = (pmine[y] + phalf[1].astype(f32)).astype(bf16)
    lump = pgot2.shape[1]
    s, v = pair()
    finish = exchange(
        nr, r, line, lambda d: lined(psum, d * lump, lump), lambda k: pgot2.at[k], lambda k: pgot2.at[k], s, v
    )
    pgot2[r] = psum[pl.ds(pl.multiple_of(r * lump, 16), lump), :]
    finish()
    pall[pl.ds(pl.multiple_of(r * lump, 16), lump), :] = sum(
        (pgot2[k].astype(f32) for k in range(1, nr)), pgot2[0].astype(f32)
    ).astype(bf16)
    def pspot(k):
        return lined(pall, k * lump, lump)
    s, v = pair()
    exchange(nr, r, line, lambda d: pspot(r), lambda k: pspot(r), pspot, s, v)()
    projected[...] = pall[...].astype(f32)

    placed.wait()
    finish_early()
    finish_late()
    pl.when(flat < last)(lambda: halo(0).wait_send())
    pl.when(flat > 0)(lambda: halo(1).wait_send())
    for n in range(len(chunks)):
        cross(n).wait_send()
    pl.when(r < nr - 1)(lambda: down().wait_send())
    pl.when(r > 0)(lambda: up().wait_send())
    for j in (0, 1):
        for s in range(3):
            each(j, s, lambda step: to_mate(j, s, step).wait_send())


def shards(nr, nc, basis, lower, diag, upper, inverse):
    blocks, size, _ = diag.shape
    width = basis.shape[1]
    h = nc // 2
    half = width * h
    order = 2 * half
    count = blocks // nc
    across = half // LANES
    body = count * size
    f32, bf16 = jnp.float32, jnp.bfloat16

    def parcel(lines, parts):
        piece = -(-lines // (h * parts * 8)) * 8
        return piece * parts, piece

    share, piece = parcel(across * (across + 1) // 2 * LANES, nr)
    xshare, xpiece = parcel(across * half, 2 * nr)
    lump = order // nr
    dma = pltpu.SemaphoreType.DMA
    pair = lambda n: [dma((n,)), dma((n,))]
    held = [pltpu.VMEM((2, count, size, size), bf16)] * 4
    bext = (2, (count + 2) * size, half)
    ext = ((count + 2) * size, order)
    chunks = (count - 2) // 2 + 2
    square = pltpu.VMEM((half, half), f32)
    opflops = 16 * count * size * size * order + 6 * count * size * order * order
    return pl.pallas_call(
        functools.partial(whole_kernel, nr, nc),
        out_shape=(
            jax.ShapeDtypeStruct(basis.shape, bf16),
            jax.ShapeDtypeStruct((order, width), f32),
        ),
        in_specs=[ANY] * 5,
        out_specs=(ANY, VMEM),
        scratch_shapes=[
            pltpu.VMEM(bext, bf16), pltpu.VMEM(ext, bf16), pltpu.VMEM((body, half), bf16), pltpu.VMEM(ext, bf16),
        ] + held + [
            square, square, pltpu.VMEM((order, order), f32), pltpu.VMEM((order, order), bf16),
            pltpu.VMEM((across, LANES, 2 * half), f32), pltpu.VMEM((across, LANES, LANES), f32),
            square, square, square,
            pltpu.VMEM((h * share, LANES), f32), pltpu.VMEM((h, share, LANES), f32), pltpu.VMEM((share, LANES), f32),
            pltpu.VMEM((nr, piece, LANES), f32), pltpu.VMEM((2, h * share, LANES), f32),
            pltpu.VMEM((h * xshare, LANES), f32), pltpu.VMEM((h, xshare, LANES), f32), pltpu.VMEM((xshare, LANES), f32),
            pltpu.VMEM((2 * nr, xpiece, LANES), f32), pltpu.VMEM((h * xshare, LANES), f32),
            pltpu.VMEM((2, order, width), f32), pltpu.VMEM((h, 2, order, width), bf16),
            pltpu.VMEM((2, order, width), bf16), pltpu.VMEM((nr, lump, width), bf16),
            pltpu.VMEM((order, width), bf16), pltpu.VMEM((2, h, order, width), bf16),
            pltpu.VMEM((8, LANES), f32), pltpu.VMEM((order, width), bf16),
            dma((2, 4)), dma((2, 3)), dma((2, 3, h)), dma((2, 3, h)), dma((2,)),
            dma((chunks,)), dma((chunks,)), dma((2,)), dma((2,)), dma,
        ] + pair(h) + pair(nr) + pair(2 * nr) + pair(h)
        + pair(h) + pair(2 * nr) + pair(2 * nr) + pair(h)
        + pair(nc) + pair(h) + pair(1) + pair(nc) + pair(nr) + pair(nr),
        compiler_params=pltpu.CompilerParams(has_side_effects=True, collective_id=1),
        cost_estimate=pl.CostEstimate(flops=opflops, bytes_accessed=1 << 24, transcendentals=0),
        name="krylov",
    )(basis, lower, diag, upper, inverse)


def solution(mesh):
    in_specs = (
        P("rows", "cols"),
        P("rows", None, None),
        P("rows", None, None),
        P("rows", None, None),
        P("rows", None, None),
    )
    out_specs = (P("rows", "cols"), P(None, "cols"))
    body = functools.partial(shards, mesh.shape["rows"], mesh.shape["cols"])
    return jax.shard_map(body, mesh=mesh, in_specs=in_specs, out_specs=out_specs, check_vma=False)
```

```python
import functools

import jax
import jax.numpy as jnp
from jax import lax
from jax.experimental import pallas as pl
from jax.experimental.pallas import tpu as pltpu
from jax.sharding import PartitionSpec as P

LANES = 128
MESH = pl.DeviceIdType.MESH
VMEM = pl.BlockSpec(memory_space=pltpu.VMEM)
ANY = pl.BlockSpec(memory_space=pl.ANY)
SUB = 8
HI = lax.Precision.HIGHEST

def factor_tile(block):
    size = block.shape[0]
    wide = (SUB, size)
    tiles = size // SUB
    row_of = lax.broadcasted_iota(jnp.int32, wide, 0)
    lane_of = lax.broadcasted_iota(jnp.int32, wide, 1)
    a = [block[t * SUB:(t + 1) * SUB, :] for t in range(tiles)]
    out = []
    for t in range(tiles):
        base = t * SUB
        at = a[t]
        inside = (lane_of >= base) & (lane_of < base + SUB)
        unity = jnp.where(lane_of == row_of + base, 1.0, 0.0).astype(jnp.float32)
        mixed = jnp.where(inside, unity, at)
        pivot = {}
        for i in range(SUB):
            for j in range(i + 1):
                pivot[i, j] = jnp.broadcast_to(at[i:i + 1, base + j:base + j + 1], wide)
        rows = [jnp.broadcast_to(mixed[i:i + 1, :], wide) for i in range(SUB)]
        last = t == tiles - 1
        unit = {}
        solved = [None] * SUB
        fin = jnp.zeros(wide, jnp.float32)
        for j in range(SUB):
            d = pivot[j, j]
            root = lax.rsqrt(d)
            inv = 1.0 / d
            fin = jnp.where(row_of == j, rows[j] * root, fin)
            for i in range(j + 1, SUB):
                unit[i, j] = pivot[i, j] * inv
            for i in range(j + 1, SUB):
                for q in range(j + 1, i + 1):
                    pivot[i, q] = pivot[i, q] - unit[i, j] * pivot[q, j]
            for i in range(j + 1, SUB):
                rows[i] = rows[i] - unit[i, j] * rows[j]
            if not last:
                solved[j] = rows[j] * inv
        out.append(jnp.where(lane_of < base + SUB, fin, 0.0))
        if last:
            break
        for j in range(SUB - 1, -1, -1):
            for i in range(j):
                solved[i] = solved[i] - unit[j, i] * solved[j]
        for s in range(t + 1, tiles):
            new = jnp.where(inside, 0.0, a[s])
            for j in range(SUB - 1, -1, -1):
                c = jnp.broadcast_to(a[s][:, base + j:base + j + 1], wide)
                new = new - c * solved[j]
            a[s] = new
    return jnp.concatenate(out, axis=0)


def eliminate(work_ref, b, out_ref, panel_ref):
    n, size, _ = work_ref.shape
    order = n * size
    at = [work_ref[b, :, i * size:(i + 1) * size] for i in range(n)]
    block = at[0]
    for i in range(1, n):
        block = jnp.where(b == i, at[i], block)
    linv = factor_tile(block)
    live = pl.ds(pl.multiple_of(b * size, size), order + size)
    work_ref[b, :, live] = fine(linv, work_ref[b, :, live])
    for i in range(n):
        panel_ref[i] = work_ref[b, :, i * size:(i + 1) * size]

    def below(i, c):
        work_ref[i, :, live] = work_ref[i, :, live] - fine(panel_ref[i], work_ref[b, :, live], ((0,), (0,)))
        return c

    lax.fori_loop(b + 1, n, below, 0)
    out_ref[pl.ds(pl.multiple_of(b * size, size), size), :] = work_ref[b, :, order:]


def augment(work_ref):
    n, size, _ = work_ref.shape
    order = n * size
    row = lax.broadcasted_iota(jnp.int32, (size, order), 0)
    lane = lax.broadcasted_iota(jnp.int32, (size, order), 1)
    for i in range(n):
        work_ref[i, :, :order] = jnp.zeros((size, order), jnp.float32)
        work_ref[i, :, order:] = jnp.where(lane == row + i * size, 1.0, 0.0).astype(jnp.float32)


def dot(left, right):
    return jnp.dot(left, right, preferred_element_type=jnp.float32)


def inner(left, right):
    return lax.dot_general(
        left, right, (((0,), (0,)), ((), ())), preferred_element_type=jnp.float32
    )


def fine(left, right, dims=((1,), (0,))):
    return lax.dot_general(
        left, right, (dims, ((), ())), precision=HI, preferred_element_type=jnp.float32
    )


def remote(src, dst, send, recv, **where):
    return pltpu.make_async_remote_copy(
        src_ref=src, dst_ref=dst, send_sem=send, recv_sem=recv, device_id=where, device_id_type=MESH
    )


def exchange(count, me, where, source, target, arrived, send, recv):
    for step in range(1, count):
        peer = lax.rem(me + step, count)
        remote(source(peer), target(me), send.at[step], recv.at[me], **where(peer)).start()

    def finish():
        for step in range(1, count):
            peer = lax.rem(me + step, count)
            remote(
                source(peer), arrived(peer), send.at[step], recv.at[peer], **where(peer)
            ).wait()

    return finish


def around(nr, nc, r, c):
    h = nc // 2
    for step in range(1, nc):
        yield True, r, lax.rem(c + step, nc)
    for by in (1, -1):
        there = (r + by >= 0) & (r + by < nr)
        for k in range(h):
            yield there, r + by, (c // h) * h + k
    for by in (2, -2):
        yield (r + by >= 0) & (r + by < nr), r + by, c


def rounds(nr, nc):
    h = nc // 2
    seen, edge, far = {(0, 0)}, {(0, 0)}, 0
    while len(seen) < nr * nc:
        new = set()
        for r, c in edge:
            new |= {(r, k) for k in range(nc)}
            new |= {(r + by, c // h * h + k) for by in (1, -1) for k in range(h)}
            new |= {(r + by, c) for by in (2, -2)}
        edge = {d for d in new if 0 <= d[0] < nr} - seen
        seen |= edge
        far += 1
    return far


def tell(sem, nr, nc, r, c):
    for there, row, col in around(nr, nc, r, c):
        def signal():
            pl.semaphore_signal(sem, inc=1, device_id=dict(rows=row, cols=col), device_id_type=MESH)

        if there is True:
            signal()
        else:
            pl.when(there)(signal)


def hear(sem, nr, nc, r, c):
    pl.semaphore_wait(sem, sum(1 if t is True else t.astype(jnp.int32) for t, _, _ in around(nr, nc, r, c)))


def lined(ref, start, extent):
    return ref.at[pl.ds(pl.multiple_of(start, 8), extent), :]


def summed(ref, count):
    return sum((ref[k] for k in range(1, count)), ref[0])


def whole_kernel(
    nr, nc, basis, lower, diag, upper, inverse, ortho, projected,
    bext, wext, wsend, oext, wl, wd, wu, wi, gy, gx, total, rinv, cwork, cpanel, linv0, linv1, tall,
    ypack, ygot1, ypart, ygot2, yall, xpack, xgot1, xpart, xgot2, xall,
    pmine, pgot1, phalf, pgot2, psum, ppack, pgot3, pall,
    far, home, zext,
    known, wsem, lsem, bsend, brecv, esem, osem, orecv, hsend, hrecv, fsend, frecv, isem, msend, mrecv, *sems,
):
    sems = list(sems)

    def pair():
        return sems.pop(0), sems.pop(0)

    bf16, f32 = jnp.bfloat16, jnp.float32
    r, c = lax.axis_index("rows"), lax.axis_index("cols")
    h = nc // 2
    y, p = c // h, lax.rem(c, h)
    other = (1 - y) * h + p
    _, count, size, _ = wl.shape
    width = basis.shape[1]
    half = width * h
    order = 2 * half
    body = count * size
    bottom = size + body
    team = 2 * nr
    seat = 2 * r + y

    def mate(k):
        return dict(cols=y * h + k)

    def member(k):
        return dict(rows=k // 2, cols=lax.rem(k, 2) * h + p)

    def line(k):
        return dict(rows=k)

    def at(i):
        return pl.ds(pl.multiple_of(i * size, size), size)

    def lanes(k, extent):
        return pl.ds(pl.multiple_of(k * extent, LANES), extent)

    weights = []
    for j, g in enumerate((other, c)):
        batch = [
            pltpu.make_async_copy(part.at[pl.ds(g * count, count)], held.at[j], wsem.at[j, k])
            for k, (part, held) in enumerate(zip((lower, diag, upper, inverse), (wl, wd, wu, wi)))
        ]
        for copy in batch:
            copy.start()
        weights.append(batch)

    spans = [(0, size), (size, body), (bottom, size)]

    def group(j, k):
        return y * h + k if j else (1 - y) * h + k

    def leaving(j, s, k):
        start, extent = spans[s]
        return basis.at[pl.ds(pl.multiple_of(group(j, k) * body - size + start, size), extent), :]

    def landing(j, s, k):
        start, extent = spans[s]
        return bext.at[j, pl.ds(start, extent), lanes(k, width)]

    def within(s, g, action):
        if s == 0:
            pl.when(g > 0)(action)
        elif s == 2:
            pl.when(g < nc - 1)(action)
        else:
            action()

    def own(j, s):
        return pltpu.make_async_copy(leaving(j, s, p), landing(j, s, p), lsem.at[j, s])

    def to_mate(j, s, step):
        k = lax.rem(p + step, h)
        return remote(leaving(j, s, k), landing(j, s, p), bsend.at[j, s, step], brecv.at[j, s, p], **mate(k))

    def down():
        return remote(
            basis.at[pl.ds(nc * body - size, size), :], landing(1 - y, 0, p), esem.at[0],
            brecv.at[1 - y, 0, p], rows=r + 1, cols=y * h,
        )

    def up():
        return remote(
            basis.at[pl.ds(0, size), :], landing(y, 2, p), esem.at[1],
            brecv.at[y, 2, p], rows=r - 1, cols=y * h + h - 1,
        )

    for j in (0, 1):
        for s in (1, 0, 2):
            within(s, group(j, p), lambda: own(j, s).start())

    barrier = pltpu.get_barrier_semaphore()
    tell(barrier, nr, nc, r, c)
    hear(barrier, nr, nc, r, c)
    heard = known.shape[0]
    tell(known.at[0], nr, nc, r, c)
    told = [0]

    def spread():
        if told[0] < heard:
            hear(known.at[told[0]], nr, nc, r, c)
            told[0] += 1
            if told[0] < heard:
                tell(known.at[told[0]], nr, nc, r, c)

    def each(j, s, action):
        for step in range(1, h):
            k = lax.rem(p + step, h)
            within(s, group(j, k), functools.partial(action, step))

    for step in range(1, h):
        to_mate(0, 1, step).start()
    pl.when(r < nr - 1)(lambda: down().start())
    pl.when(r > 0)(lambda: up().start())
    for j, s in ((0, 0), (0, 2), (1, 1), (1, 0), (1, 2)):
        each(j, s, lambda step: to_mate(j, s, step).start())

    for j in (0, 1):
        @pl.when((r == 0) & (group(j, p) == 0))
        def _():
            bext[j, 0:size, :] = jnp.zeros((size, half), bf16)

        @pl.when((r == nr - 1) & (group(j, p) == nc - 1))
        def _():
            bext[j, bottom:bottom + size, :] = jnp.zeros((size, half), bf16)

    @pl.when((r == 0) & (c == 0))
    def _():
        wext[0:size, :] = jnp.zeros((size, order), bf16)

    @pl.when((r == nr - 1) & (c == nc - 1))
    def _():
        wext[bottom:bottom + size, :] = jnp.zeros((size, order), bf16)

    def arrive(j, s):
        g = group(j, p)
        within(s, g, lambda: own(j, s).wait())
        for k in range(h):
            comes = k != p
            if s == 0:
                comes = ((g > 0) & comes) | ((g == 0) & (r > 0))
            elif s == 2:
                comes = ((g < nc - 1) & comes) | ((g == nc - 1) & (r < nr - 1))
            extent = spans[s][1]
            pl.when(comes)(
                lambda: remote(
                    basis.at[pl.ds(0, extent), :], landing(j, s, k), bsend.at[j, s, 0], brecv.at[j, s, k], **mate(k)
                ).wait_recv()
            )

    def applied(field, j, i, columns):
        mixed = (
            dot(wl[j, i], field[i * size:(i + 1) * size, columns])
            + dot(wd[j, i], field[(i + 1) * size:(i + 2) * size, columns])
            + dot(wu[j, i], field[(i + 2) * size:(i + 3) * size, columns])
        )
        return dot(wi[j, i], mixed.astype(bf16)).astype(bf16)

    mine = lanes(y, half)
    chunks = [(i, 2) for i in range(1, count - 1, 2)] + [(0, 1), (count - 1, 1)]

    def cross(n, to=None):
        start, extent = chunks[n][0] * size, chunks[n][1] * size
        return remote(
            wsend.at[pl.ds(start, extent), :],
            wext.at[pl.ds(size + start, extent), mine if to is None else to],
            osem.at[n], orecv.at[n], cols=other,
        )

    gy[...] = jnp.zeros_like(gy)
    for copy in weights[0]:
        copy.wait()
    arrive(0, 1)
    held_back = max(len(chunks) - 3, 1)
    for n, (first, extent) in enumerate(chunks):
        if first == 0:
            arrive(0, 0)
            arrive(0, 2)
        ws = []
        for i in range(first, first + extent):
            w = applied(bext.at[0], 0, i, slice(None))
            wsend[i * size:(i + 1) * size, :] = w
            ws.append(w)
        if n < held_back:
            cross(n).start()
        gy[...] += sum(inner(w, w) for w in ws)
        if n:
            spread()
    for copy in weights[1]:
        copy.wait()
    arrive(1, 1)

    def second(some):
        ws = []
        for i in some:
            w = applied(bext.at[1], 1, i, slice(None))
            wext[(i + 1) * size:(i + 2) * size, mine] = w
            ws.append(w)
        gy[...] += sum(inner(w, w) for w in ws)

    second(range(1, count // 2))
    spread()
    second(range(count // 2, count - 1))
    arrive(1, 0)
    arrive(1, 2)
    second((0, count - 1))
    for _ in range(heard):
        spread()

    across = half // LANES
    place = 0
    for i in range(across):
        for j in range(i, across):
            ypack[place * LANES:(place + 1) * LANES, :] = gy[
                i * LANES:(i + 1) * LANES, j * LANES:(j + 1) * LANES
            ]
            place += 1
    if ypack.shape[0] > place * LANES:
        ypack[place * LANES:, :] = jnp.zeros((ypack.shape[0] - place * LANES, LANES), f32)
    share, piece = ygot1.shape[1], ygot2.shape[1]
    s, v = pair()
    finish = exchange(
        h, p, mate, lambda d: lined(ypack, d * share, share), lambda k: ygot1.at[k], lambda k: ygot1.at[k], s, v
    )
    ygot1[p] = ypack[pl.ds(pl.multiple_of(p * share, 8), share), :]
    finish()
    ypart[...] = summed(ygot1, h)
    s, v = pair()
    finish = exchange(
        nr, r, line, lambda d: lined(ypart, d * piece, piece), lambda k: ygot2.at[k], lambda k: ygot2.at[k], s, v
    )
    ygot2[r] = ypart[pl.ds(pl.multiple_of(r * piece, 8), piece), :]
    finish()
    def yspot(k):
        return yall.at[lax.rem(k, 2), pl.ds(pl.multiple_of(p * share + (k // 2) * piece, 8), piece), :]
    yall[y, pl.ds(pl.multiple_of(p * share + r * piece, 8), piece), :] = summed(ygot2, nr)
    s, v = pair()
    finish = exchange(team, seat, member, lambda d: yspot(seat), lambda k: yspot(seat), yspot, s, v)
    for n in range(held_back, len(chunks)):
        cross(n).start()
    finish()
    def yshare(k):
        return yall.at[:, pl.ds(pl.multiple_of(k * share, 8), share), :]
    s, v = pair()
    exchange(h, p, mate, lambda d: yshare(p), lambda k: yshare(p), yshare, s, v)()

    def load(which):
        place = 0
        for i in range(across):
            for j in range(i, across):
                cwork[i, :, j * LANES:(j + 1) * LANES] = yall[which, place * LANES:(place + 1) * LANES, :]
                place += 1

    flat = r * nc + c
    last = nr * nc - 1

    def halo(kind):
        start = (body, size)[kind]
        target = (0, bottom)[kind]
        to = flat + (1, -1)[kind]
        return remote(
            wext.at[pl.ds(start, size), :], wext.at[pl.ds(target, size), :], hsend.at[kind], hrecv.at[kind],
            rows=to // nc, cols=lax.rem(to, nc),
        )


    def further(n):
        start, extent = chunks[n][0] * size, chunks[n][1] * size
        return remote(
            wext.at[pl.ds(size + start, extent), :half], far.at[pl.ds(start, extent), :],
            fsend.at[n], frecv.at[n], cols=other,
        )

    theirs = lanes(1 - y, half)
    xshare, xpiece = xgot1.shape[1], xgot2.shape[1]
    def xspot(k):
        return lined(xall, p * xshare + k * xpiece, xpiece)
    def xsection(k):
        return lined(xall, k * xshare, xshare)
    xcore, xscatter, xgather, xcopy = pair(), pair(), pair(), pair()

    def scatter():
        return exchange(
            team, seat, member, lambda d: lined(xpart, d * xpiece, xpiece), lambda k: xgot2.at[k],
            lambda k: xgot2.at[k], *xscatter,
        )

    def cross_half():
        gx[...] = jnp.zeros_like(gx)
        for n, (first, extent) in enumerate(chunks):
            cross(n, theirs).wait_recv()
            rows = slice((first + 1) * size, (first + 1 + extent) * size)
            gx[...] += inner(wext[rows, :half], wext[rows, half:])

        for j in range(across):
            xpack[j * half:(j + 1) * half, :] = gx[:, j * LANES:(j + 1) * LANES]
        if xpack.shape[0] > across * half:
            xpack[across * half:, :] = jnp.zeros((xpack.shape[0] - across * half, LANES), f32)
        finish = exchange(
            h, p, mate, lambda d: lined(xpack, d * xshare, xshare), lambda k: xgot1.at[k], lambda k: xgot1.at[k], *xcore
        )
        xgot1[p] = xpack[pl.ds(pl.multiple_of(p * xshare, 8), xshare), :]
        finish()
        xpart[...] = summed(xgot1, h)
        scatter()

    def whole_half():
        for step in range(1, team):
            peer = lax.rem(seat + step, team)
            remote(
                lined(xpart, peer * xpiece, xpiece), xgot2.at[peer], xscatter[0].at[step], xscatter[1].at[peer],
                **member(peer),
            ).wait()
        xgot2[seat] = xpart[pl.ds(pl.multiple_of(seat * xpiece, 8), xpiece), :]
        xall[pl.ds(pl.multiple_of(p * xshare + seat * xpiece, 8), xpiece), :] = summed(xgot2, team)
        exchange(team, seat, member, lambda d: xspot(seat), lambda k: xspot(seat), xspot, *xgather)()
        pl.when(flat < last)(lambda: halo(0).start())
        pl.when(flat > 0)(lambda: halo(1).start())

        @pl.when(y == 0)
        def _():
            for n in range(len(chunks)):
                further(n).start()

        exchange(h, p, mate, lambda d: xsection(p), lambda k: xsection(p), xsection, *xcopy)()
        for j in range(across):
            gx[:, j * LANES:(j + 1) * LANES] = xall[j * half:(j + 1) * half, :]
        linv0[...] = linv1[...]
        tall[...] = fine(linv0[...], gx[...])
        augment(cwork)
        load(1)
        for i in range(across):
            cwork[i, :, :half] = cwork[i, :, :half] - fine(
                tall[:, i * LANES:(i + 1) * LANES], tall[...], ((0,), (0,))
            )
        gx[...] = fine(tall[...], linv0[...], ((0,), (0,)))

    augment(cwork)
    load(0)

    def factor_step(g, carry):
        eliminate(cwork, lax.rem(g, across), linv1, cpanel)
        pl.when(g == 0)(cross_half)
        pl.when(g == across - 1)(whole_half)
        return carry

    lax.fori_loop(0, 2 * across, factor_step, 0)
    rinv[:half, :half] = linv0[...].T.astype(bf16)
    rinv[half:, half:] = linv1[...].T.astype(bf16)
    rinv[:half, half:] = (-fine(linv1[...], gx[...])).T.astype(bf16)

    def turn(i):
        rows = slice(i * size, (i + 1) * size)
        oext[rows, :half] = dot(wext[rows, :half], rinv[:half, :half]).astype(bf16)
        oext[rows, half:] = dot(wext[rows, :], rinv[:, half:]).astype(bf16)

    for i in range(1, count + 1):
        turn(i)
    pl.when(flat > 0)(lambda: halo(0).wait_recv())
    pl.when(flat < last)(lambda: halo(1).wait_recv())
    turn(0)
    turn(count + 1)
    for i in range(count):
        zext[i * size:(i + 1) * size, :] = applied(oext, 1, i, slice(None))
    for i in range(2):
        for k in range(2):
            ri, ck = slice(i * half, (i + 1) * half), slice(k * half, (k + 1) * half)
            total[ri, ck] = inner(oext[size:bottom, ri], zext[:, ck])

    def place(j, source, first, k):
        return source.at[pl.ds(first, body), k], ortho.at[pl.ds(pl.multiple_of((c if j else other) * body, size), body), :]

    def settle(j):
        source, first = (oext, size) if j else (home, 0)
        col = (lambda k: lanes(y * h + k, width)) if j else (lambda k: lanes(k, width))
        own_copy = pltpu.make_async_copy(*place(j, source, first, col(p)), isem.at[j])
        own_copy.start()
        moves = [own_copy]
        for step in range(1, h):
            k = lax.rem(p + step, h)
            src_ref, dst_ref = place(j, source, first, col(k))
            remote(src_ref, dst_ref, msend.at[j, step], mrecv.at[j, p], **mate(k)).start()

        def finish():
            own_copy.wait()
            for step in range(1, h):
                k = lax.rem(p + step, h)
                src_ref, dst_ref = place(j, source, first, col(k))
                sent = remote(src_ref, dst_ref, msend.at[j, step], mrecv.at[j, p], **mate(k))
                sent.wait_send()
                g = (y if j else 1 - y) * h + k
                remote(
                    src_ref, ortho.at[pl.ds(pl.multiple_of(g * body, size), body), :], msend.at[j, step],
                    mrecv.at[j, k], **mate(k),
                ).wait_recv()

        return finish

    for k in range(2):
        for q in range(h):
            ppack[k, q] = total[:, (k * h + q) * width:(k * h + q + 1) * width].astype(bf16)
    s, v = pair()
    exchange(
        h, p, mate, lambda d: ppack.at[:, d], lambda k: pgot1.at[k], lambda k: pgot1.at[k], s, v
    )()
    for k in range(2):
        pmine[k] = total[:, lanes(k * h + p, width)]
    for step in range(1, h):
        for k in range(2):
            pmine[k] = pmine[k] + pgot1[lax.rem(p + step, h), k].astype(f32)
    phalf[0] = pmine[1 - y].astype(bf16)
    s, v = pair()
    crossing = remote(phalf.at[0], phalf.at[1], s.at[0], v.at[0], cols=other)
    crossing.start()
    finish_own = settle(1)

    @pl.when(y == 0)
    def _():
        for i in range(count):
            rows = slice(i * size, (i + 1) * size)
            home[rows, :] = dot(wsend[rows, :], rinv[:half, :half]).astype(bf16)

    crossing.wait()
    psum[...] = (pmine[y] + phalf[1].astype(f32)).astype(bf16)
    lump = pgot2.shape[1]
    s, v = pair()
    finish = exchange(
        nr, r, line, lambda d: lined(psum, d * lump, lump), lambda k: pgot2.at[k], lambda k: pgot2.at[k], s, v
    )
    pgot2[r] = psum[pl.ds(pl.multiple_of(r * lump, 16), lump), :]

    @pl.when(y == 1)
    def _():
        for n in range(len(chunks)):
            further(n).wait_recv()
        for i in range(count):
            rows = slice(i * size, (i + 1) * size)
            home[rows, :] = (dot(far[rows, :], rinv[:half, half:]) + dot(wsend[rows, :], rinv[half:, half:])).astype(bf16)

    finish_other = settle(0)
    finish()
    pall[pl.ds(pl.multiple_of(r * lump, 16), lump), :] = sum(
        (pgot2[k].astype(f32) for k in range(1, nr)), pgot2[0].astype(f32)
    ).astype(bf16)
    def pspot(k):
        return lined(pall, k * lump, lump)
    s, v = pair()
    exchange(nr, r, line, lambda d: pspot(r), lambda k: pspot(r), pspot, s, v)()
    projected[...] = pall[...].astype(f32)

    finish_own()
    finish_other()

    @pl.when(y == 0)
    def _():
        for n in range(len(chunks)):
            further(n).wait_send()

    pl.when(flat < last)(lambda: halo(0).wait_send())
    pl.when(flat > 0)(lambda: halo(1).wait_send())
    for n in range(len(chunks)):
        cross(n).wait_send()
    pl.when(r < nr - 1)(lambda: down().wait_send())
    pl.when(r > 0)(lambda: up().wait_send())
    for j in (0, 1):
        for s in range(3):
            each(j, s, lambda step: to_mate(j, s, step).wait_send())


def shards(nr, nc, basis, lower, diag, upper, inverse):
    blocks, size, _ = diag.shape
    width = basis.shape[1]
    h = nc // 2
    half = width * h
    order = 2 * half
    count = blocks // nc
    across = half // LANES
    body = count * size
    f32, bf16 = jnp.float32, jnp.bfloat16

    def parcel(lines, parts):
        piece = -(-lines // (h * parts * 8)) * 8
        return piece * parts, piece

    share, piece = parcel(across * (across + 1) // 2 * LANES, nr)
    xshare, xpiece = parcel(across * half, 2 * nr)
    lump = order // nr
    dma = pltpu.SemaphoreType.DMA
    pair = lambda n: [dma((n,)), dma((n,))]
    held = [pltpu.VMEM((2, count, size, size), bf16)] * 4
    bext = (2, (count + 2) * size, half)
    ext = ((count + 2) * size, order)
    chunks = (count - 2) // 2 + 2
    square = pltpu.VMEM((half, half), f32)
    opflops = 16 * count * size * size * order + 6 * count * size * order * order
    return pl.pallas_call(
        functools.partial(whole_kernel, nr, nc),
        out_shape=(pltpu.VMEM(basis.shape, bf16), pltpu.VMEM((order, width), f32)),
        in_specs=[ANY] * 5,
        out_specs=(VMEM, VMEM),
        scratch_shapes=[
            pltpu.VMEM(bext, bf16), pltpu.VMEM(ext, bf16), pltpu.VMEM((body, half), bf16), pltpu.VMEM(ext, bf16),
        ] + held + [
            square, square, pltpu.VMEM((order, order), f32), pltpu.VMEM((order, order), bf16),
            pltpu.VMEM((across, LANES, 2 * half), f32), pltpu.VMEM((across, LANES, LANES), f32),
            square, square, square,
            pltpu.VMEM((h * share, LANES), f32), pltpu.VMEM((h, share, LANES), f32), pltpu.VMEM((share, LANES), f32),
            pltpu.VMEM((nr, piece, LANES), f32), pltpu.VMEM((2, h * share, LANES), f32),
            pltpu.VMEM((h * xshare, LANES), f32), pltpu.VMEM((h, xshare, LANES), f32), pltpu.VMEM((xshare, LANES), f32),
            pltpu.VMEM((2 * nr, xpiece, LANES), f32), pltpu.VMEM((h * xshare, LANES), f32),
            pltpu.VMEM((2, order, width), f32), pltpu.VMEM((h, 2, order, width), bf16),
            pltpu.VMEM((2, order, width), bf16), pltpu.VMEM((nr, lump, width), bf16),
            pltpu.VMEM((order, width), bf16), pltpu.VMEM((2, h, order, width), bf16),
            pltpu.VMEM((8, LANES), f32), pltpu.VMEM((order, width), bf16),
            pltpu.VMEM((body, half), bf16), pltpu.VMEM((body, half), bf16), pltpu.VMEM((body, order), bf16),
            pltpu.SemaphoreType.REGULAR((rounds(nr, nc) - 1,)),
            dma((2, 4)), dma((2, 3)), dma((2, 3, h)), dma((2, 3, h)), dma((2,)),
            dma((chunks,)), dma((chunks,)), dma((2,)), dma((2,)), dma((chunks,)), dma((chunks,)),
            dma((2,)), dma((2, h)), dma((2, h)),
        ] + pair(h) + pair(nr) + pair(2 * nr) + pair(h)
        + pair(h) + pair(2 * nr) + pair(2 * nr) + pair(h)
        + pair(h) + pair(1) + pair(nr) + pair(nr),
        compiler_params=pltpu.CompilerParams(has_side_effects=True, collective_id=1),
        cost_estimate=pl.CostEstimate(flops=opflops, bytes_accessed=1 << 24, transcendentals=0),
        name="krylov",
    )(basis, lower, diag, upper, inverse)


def solution(mesh):
    in_specs = (
        P("rows", "cols"),
        P("rows", None, None),
        P("rows", None, None),
        P("rows", None, None),
        P("rows", None, None),
    )
    out_specs = (P("rows", "cols"), P(None, "cols"))
    body = functools.partial(shards, mesh.shape["rows"], mesh.shape["cols"])
    return jax.shard_map(body, mesh=mesh, in_specs=in_specs, out_specs=out_specs, check_vma=False)
```

```python
import functools

import jax
import jax.numpy as jnp
from jax import lax
from jax.experimental import pallas as pl
from jax.experimental.pallas import tpu as pltpu
from jax.sharding import PartitionSpec as P

LANES = 128
MESH = pl.DeviceIdType.MESH
VMEM = pl.BlockSpec(memory_space=pltpu.VMEM)
ANY = pl.BlockSpec(memory_space=pl.ANY)
SUB = 8
HI = lax.Precision.HIGHEST

def factor_tile(block, hold):
    size = block.shape[0]
    wide = (SUB, size)
    tiles = size // SUB
    row_of = lax.broadcasted_iota(jnp.int32, wide, 0)
    lane_of = lax.broadcasted_iota(jnp.int32, wide, 1)
    a = [block[t * SUB:(t + 1) * SUB, :] for t in range(tiles)]
    out = []
    for t in range(tiles):
        base = t * SUB
        at = a[t]
        last = t == tiles - 1
        inside = (lane_of >= base) & (lane_of < base + SUB)
        unity = jnp.where(lane_of == row_of + base, 1.0, 0.0).astype(jnp.float32)
        mixed = jnp.where(inside, unity, at)
        pivot = {}
        for j in range(SUB):
            hold[t % 2, j] = jnp.broadcast_to(at[:, base + j:base + j + 1], wide)
        for j in range(SUB):
            for i in range(j, SUB):
                pivot[i, j] = hold[t % 2, j, pl.ds(i, SUB, stride=0), :]
        rows = [jnp.broadcast_to(mixed[i:i + 1, :], wide) for i in range(SUB)]
        unit = {}
        solved = [None] * SUB
        if not last:
            ahead = jnp.where(inside, 0.0, a[t + 1])
            edge = [jnp.broadcast_to(a[t + 1][:, base + j:base + j + 1], wide) for j in range(SUB)]
        fin = jnp.zeros(wide, jnp.float32)
        for j in range(SUB):
            d = pivot[j, j]
            root = lax.rsqrt(d)
            inv = 1.0 / d
            for i in range(j + 1, SUB):
                unit[i, j] = pivot[i, j] * inv
            for i in range(j + 1, SUB):
                for q in range(j + 1, i + 1):
                    pivot[i, q] = pivot[i, q] - unit[i, j] * pivot[q, j]
            for i in range(j + 1, SUB):
                rows[i] = rows[i] - unit[i, j] * rows[j]
            fin = jnp.where(row_of == j, rows[j] * root, fin)
            if not last:
                solved[j] = rows[j] * inv
                ahead = ahead - edge[j] * solved[j]
                for q in range(j + 1, SUB):
                    edge[q] = edge[q] - edge[j] * unit[q, j]
        out.append(jnp.where(lane_of < base + SUB, fin, 0.0))
        if last:
            break
        a[t + 1] = ahead
        if t + 2 < tiles:
            for j in range(SUB - 1, -1, -1):
                for i in range(j):
                    solved[i] = solved[i] - unit[j, i] * solved[j]
        for s in range(t + 2, tiles):
            new = jnp.where(inside, 0.0, a[s])
            for j in range(SUB - 1, -1, -1):
                c = jnp.broadcast_to(a[s][:, base + j:base + j + 1], wide)
                new = new - c * solved[j]
            a[s] = new
    return jnp.concatenate(out, axis=0)


def eliminate(work_ref, b, out_ref, panel_ref, hold_ref):
    n, size, _ = work_ref.shape
    at = [work_ref[b, :, i * size:(i + 1) * size] for i in range(n)]
    block = at[0]
    for i in range(1, n):
        block = jnp.where(b == i, at[i], block)
    panel_ref[...] = factor_tile(block, hold_ref)

    def stage(k):
        linv = panel_ref[...]
        rows = slice(k * size, (k + 1) * size)
        if k:
            out_ref[rows, :k * size] = fine(linv, out_ref[rows, :k * size])
        out_ref[rows, rows] = linv
        if k + 1 < n:
            out_ref[rows, (k + 1) * size:] = jnp.zeros((size, (n - k - 1) * size), jnp.float32)
            right = fine(linv, work_ref[k, :, (k + 1) * size:n * size])
            known = jnp.concatenate([right, out_ref[rows, :(k + 1) * size]], axis=1)
            for i in range(k + 1, n):
                step = fine(right[:, (i - k - 1) * size:(i - k) * size], known, ((0,), (0,)))
                lines = slice(i * size, (i + 1) * size)
                cut = (n - k - 1) * size
                work_ref[i, :, (k + 1) * size:n * size] = work_ref[i, :, (k + 1) * size:n * size] - step[:, :cut]
                if k:
                    out_ref[lines, :k * size] = out_ref[lines, :k * size] - step[:, cut:cut + k * size]
                out_ref[lines, rows] = -step[:, cut + k * size:]

    for k in range(n):
        pl.when(b == k)(functools.partial(stage, k))


def dot(left, right):
    return jnp.dot(left, right, preferred_element_type=jnp.float32)


def inner(left, right):
    return lax.dot_general(
        left, right, (((0,), (0,)), ((), ())), preferred_element_type=jnp.float32
    )


def fine(left, right, dims=((1,), (0,))):
    return lax.dot_general(
        left, right, (dims, ((), ())), precision=HI, preferred_element_type=jnp.float32
    )


def remote(src, dst, send, recv, **where):
    return pltpu.make_async_remote_copy(
        src_ref=src, dst_ref=dst, send_sem=send, recv_sem=recv, device_id=where, device_id_type=MESH
    )


def exchange(count, me, where, source, target, whole, send, recv):
    for step in range(1, count):
        peer = lax.rem(me + step, count)
        remote(source(peer), target(me), send, recv, **where(peer)).start()

    def finish():
        if count > 1:
            remote(whole, whole, send, recv, **where(lax.rem(me + 1, count))).wait()

    return finish


def around(nr, nc, r, c):
    h = nc // 2
    for step in range(1, nc):
        yield True, r, lax.rem(c + step, nc)
    for by in (1, -1):
        there = (r + by >= 0) & (r + by < nr)
        for k in range(h):
            yield there, r + by, (c // h) * h + k
    for by in (2, -2):
        yield (r + by >= 0) & (r + by < nr), r + by, c


def rounds(nr, nc):
    h = nc // 2
    seen, edge, far = {(0, 0)}, {(0, 0)}, 0
    while len(seen) < nr * nc:
        new = set()
        for r, c in edge:
            new |= {(r, k) for k in range(nc)}
            new |= {(r + by, c // h * h + k) for by in (1, -1) for k in range(h)}
            new |= {(r + by, c) for by in (2, -2)}
        edge = {d for d in new if 0 <= d[0] < nr} - seen
        seen |= edge
        far += 1
    return far


def tell(sem, nr, nc, r, c):
    for there, row, col in around(nr, nc, r, c):
        def signal():
            pl.semaphore_signal(sem, inc=1, device_id=dict(rows=row, cols=col), device_id_type=MESH)

        if there is True:
            signal()
        else:
            pl.when(there)(signal)


def hear(sem, nr, nc, r, c):
    pl.semaphore_wait(sem, sum(1 if t is True else t.astype(jnp.int32) for t, _, _ in around(nr, nc, r, c)))


def lined(ref, start, extent):
    return ref.at[pl.ds(pl.multiple_of(start, 8), extent), :]


def summed(ref, count):
    return sum((ref[k] for k in range(1, count)), ref[0])


def whole_kernel(
    nr, nc, basis, lower, diag, upper, inverse, ortho, projected,
    bext, wext, wsend, oext, held, gy, gx, total, rinv, cwork, cpanel, hold, linv0, linv1, tall,
    ypack, ygot1, ypart, ygot2, yall, xpack, xgot1, xpart, xgot2, xall,
    pgot1, phalf, pgot2, psum, ppack, pall,
    far, home, zext, mix,
    known, wsem, bsend, brecv, esem, osem, orecv, hsend, hrecv, fsend, frecv, isem, msend, mrecv, *sems,
):
    sems = list(sems)

    def pair():
        return sems.pop(0), sems.pop(0)

    bf16, f32 = jnp.bfloat16, jnp.float32
    r, c = lax.axis_index("rows"), lax.axis_index("cols")
    h = nc // 2
    y, p = c // h, lax.rem(c, h)
    other = (1 - y) * h + p
    _, _, count, size, _ = held.shape
    width = basis.shape[1]
    half = width * h
    order = 2 * half
    body = count * size
    bottom = size + body
    team = 2 * nr
    seat = 2 * r + y

    def mate(k):
        return dict(cols=y * h + k)

    def member(k):
        return dict(rows=k // 2, cols=lax.rem(k, 2) * h + p)

    def line(k):
        return dict(rows=k)

    def at(i):
        return pl.ds(pl.multiple_of(i * size, size), size)

    def lanes(k, extent):
        return pl.ds(pl.multiple_of(k * extent, LANES), extent)

    wl, wd, wu, wi = (held.at[:, k] for k in range(4))
    for j, g in enumerate((other, c)):
        for k, part in enumerate((lower, diag, upper, inverse)):
            pltpu.make_async_copy(part.at[pl.ds(g * count, count)], held.at[j, k], wsem.at[j]).start()

    def weighed(j):
        pltpu.make_async_copy(held.at[1 - j], held.at[j], wsem.at[j]).wait()

    spans = [(0, size), (size, body), (bottom, size)]

    def group(j, k):
        return y * h + k if j else (1 - y) * h + k

    def leaving(j, s, k):
        start, extent = spans[s]
        return basis.at[pl.ds(pl.multiple_of(group(j, k) * body - size + start, size), extent), :]

    def landing(j, s, k):
        start, extent = spans[s]
        return bext.at[j, pl.ds(start, extent), lanes(k, width)]

    def within(s, g, action):
        if s == 0:
            pl.when(g > 0)(action)
        elif s == 2:
            pl.when(g < nc - 1)(action)
        else:
            action()

    def own(j, s):
        return pltpu.make_async_copy(leaving(j, s, p), landing(j, s, p), brecv.at[j, s])

    def to_mate(j, s, step):
        k = lax.rem(p + step, h)
        return remote(leaving(j, s, k), landing(j, s, p), bsend.at[j, s], brecv.at[j, s], **mate(k))

    def down():
        return remote(
            basis.at[pl.ds(nc * body - size, size), :], landing(1 - y, 0, p), esem.at[0],
            brecv.at[1 - y, 0], rows=r + 1, cols=y * h,
        )

    def up():
        return remote(
            basis.at[pl.ds(0, size), :], landing(y, 2, p), esem.at[1],
            brecv.at[y, 2], rows=r - 1, cols=y * h + h - 1,
        )

    for j in (0, 1):
        for s in (1, 0, 2):
            within(s, group(j, p), lambda: own(j, s).start())

    barrier = pltpu.get_barrier_semaphore()
    tell(barrier, nr, nc, r, c)
    hear(barrier, nr, nc, r, c)
    heard = known.shape[0]
    tell(known.at[0], nr, nc, r, c)
    told = [0]

    def spread():
        if told[0] < heard:
            hear(known.at[told[0]], nr, nc, r, c)
            told[0] += 1
            if told[0] < heard:
                tell(known.at[told[0]], nr, nc, r, c)

    def each(j, s, action):
        for step in range(1, h):
            k = lax.rem(p + step, h)
            within(s, group(j, k), functools.partial(action, step))

    for step in range(1, h):
        to_mate(0, 1, step).start()
    pl.when(r < nr - 1)(lambda: down().start())
    pl.when(r > 0)(lambda: up().start())
    for j, s in ((0, 0), (0, 2), (1, 1), (1, 0), (1, 2)):
        each(j, s, lambda step: to_mate(j, s, step).start())

    for j in (0, 1):
        @pl.when((r == 0) & (group(j, p) == 0))
        def _():
            bext[j, 0:size, :] = jnp.zeros((size, half), bf16)

        @pl.when((r == nr - 1) & (group(j, p) == nc - 1))
        def _():
            bext[j, bottom:bottom + size, :] = jnp.zeros((size, half), bf16)

    @pl.when((r == 0) & (c == 0))
    def _():
        wext[0:size, :] = jnp.zeros((size, order), bf16)

    @pl.when((r == nr - 1) & (c == nc - 1))
    def _():
        wext[bottom:bottom + size, :] = jnp.zeros((size, order), bf16)

    def arrive(j, s):
        g = group(j, p)
        start, extent = spans[s]
        full = bext.at[j, pl.ds(start, extent), :]
        comes = {0: (g > 0) | (r > 0), 1: r >= 0, 2: (g < nc - 1) | (r < nr - 1)}[s]
        pl.when(comes)(lambda: pltpu.make_async_copy(bext.at[1 - j, pl.ds(start, extent), :], full, brecv.at[j, s]).wait())

    def applied(field, j, some, columns, out):
        for i in some:
            mixed = (
                dot(wl[j, i], field[i * size:(i + 1) * size, columns])
                + dot(wd[j, i], field[(i + 1) * size:(i + 2) * size, columns])
                + dot(wu[j, i], field[(i + 2) * size:(i + 3) * size, columns])
            )
            mix[j, i * size:(i + 1) * size, :] = mixed.astype(bf16)
        for i in some:
            out(i, dot(wi[j, i], mix[j, i * size:(i + 1) * size, :]).astype(bf16))

    mine = lanes(y, half)
    chunks = [(1, 1), (2, 1)] + [(i, 2) for i in range(3, count - 1, 2)] + [(0, 1), (count - 1, 1)]

    def cross(n, to=None):
        start, extent = chunks[n][0] * size, chunks[n][1] * size
        return remote(
            wsend.at[pl.ds(start, extent), :],
            wext.at[pl.ds(size + start, extent), mine if to is None else to],
            osem, orecv, cols=other,
        )

    weighed(0)
    arrive(0, 1)

    def first(some):
        def keep(i, w):
            wsend[i * size:(i + 1) * size, :] = w

        applied(bext.at[0], 0, some, slice(None), keep)

    def second(some):
        def keep(i, w):
            wext[(i + 1) * size:(i + 2) * size, mine] = w

        applied(bext.at[1], 1, some, slice(None), keep)

    for n in range(len(chunks) - 2):
        start, extent = chunks[n]
        first(range(start, start + extent))
        cross(n).start()
        if n == 1:
            spread()
    weighed(1)
    arrive(1, 1)
    second(range(1, count - 1))
    spread()
    mid = slice(size, body - size)
    gy[...] = inner(wsend[mid, :], wsend[mid, :])
    spread()
    own_half = wext[2 * size:body, mine]
    gy[...] += inner(own_half, own_half)
    arrive(0, 0)
    arrive(0, 2)
    first((0, count - 1))
    for n in range(len(chunks) - 2, len(chunks)):
        cross(n).start()
    spread()
    arrive(1, 0)
    arrive(1, 2)
    second((0, count - 1))
    for _ in range(heard):
        spread()
    for rows in (slice(0, size), slice(body - size, body)):
        own_half = wext[rows.start + size:rows.stop + size, mine]
        gy[...] += inner(wsend[rows, :], wsend[rows, :]) + inner(own_half, own_half)

    early = list(range(len(chunks) // 2))
    late = sorted(range(len(chunks) // 2, len(chunks)), key=lambda n: chunks[n][1])

    def further(n):
        start, extent = chunks[n][0] * size, chunks[n][1] * size
        if n in early:
            source, target = wext.at[pl.ds(size + start, extent), :half], far.at[pl.ds(start, extent), :]
        else:
            source, target = oext.at[1, pl.ds(size + start, extent), :], home.at[pl.ds(start, extent), :]
        return remote(source, target, fsend.at[int(n in late)], frecv.at[int(n in late)], cols=other)

    def all_further(kind):
        some = (early, late)[kind]
        extent = sum(chunks[n][1] for n in some) * size
        part = far.at[pl.ds(0, extent), :]
        return remote(part, part, fsend.at[kind], frecv.at[kind], cols=other)

    def send_late(some):
        for n in some:
            further(n).start()

    across = half // LANES
    place = 0
    for i in range(across):
        for j in range(i, across):
            ypack[place * LANES:(place + 1) * LANES, :] = gy[
                i * LANES:(i + 1) * LANES, j * LANES:(j + 1) * LANES
            ]
            place += 1
    if ypack.shape[0] > place * LANES:
        ypack[place * LANES:, :] = jnp.zeros((ypack.shape[0] - place * LANES, LANES), f32)
    share, piece = ygot1.shape[1], ygot2.shape[1]
    s, v = pair()
    finish = exchange(
        h, p, mate, lambda d: lined(ypack, d * share, share), lambda k: ygot1.at[k],
        ygot1.at[pl.ds(0, h - 1)], s, v
    )
    ygot1[p] = ypack[pl.ds(pl.multiple_of(p * share, 8), share), :]
    finish()
    ypart[...] = summed(ygot1, h)
    s, v = pair()
    finish = exchange(
        nr, r, line, lambda d: lined(ypart, d * piece, piece), lambda k: ygot2.at[k],
        ygot2.at[pl.ds(0, nr - 1)], s, v
    )
    ygot2[r] = ypart[pl.ds(pl.multiple_of(r * piece, 8), piece), :]
    finish()

    def yspot(k):
        return yall.at[y, pl.ds(pl.multiple_of(p * share + k * piece, 8), piece), :]

    def yshare(side, k):
        return yall.at[side, pl.ds(pl.multiple_of(k * share, 8), share), :]

    yall[y, pl.ds(pl.multiple_of(p * share + r * piece, 8), piece), :] = summed(ygot2, nr)
    s, v = pair()
    exchange(nr, r, line, lambda d: yspot(r), lambda k: yspot(r), ygot2.at[pl.ds(0, nr - 1)], s, v)()
    s, v = pair()
    over = remote(yshare(y, p), yshare(y, p), s, v, cols=other)
    over.start()

    def both(side, sems_of):
        rest = yall.at[side, pl.ds(0, (h - 1) * share), :]
        exchange(h, p, mate, lambda d: yshare(side, p), lambda k: yshare(side, p), rest, *sems_of)()

    both(y, pair())
    opposite_sems = pair()

    def opposite():
        over.wait_recv()
        both(1 - y, opposite_sems)

    def load(which):
        place = 0
        for i in range(across):
            for j in range(i, across):
                cwork[i, :, j * LANES:(j + 1) * LANES] = yall[which, place * LANES:(place + 1) * LANES, :]
                place += 1

    flat = r * nc + c
    last = nr * nc - 1

    def halo(kind, q):
        start = (body, size)[kind]
        target = (0, bottom)[kind]
        to = flat + (1, -1)[kind]
        part = pl.ds(q * half, half)
        return remote(
            wext.at[pl.ds(start, size), part], wext.at[pl.ds(target, size), part], hsend.at[kind, q],
            hrecv.at[kind, q], rows=to // nc, cols=lax.rem(to, nc),
        )


    theirs = lanes(1 - y, half)
    xshare, xpiece = xgot1.shape[1], xgot2.shape[1]
    def xspot(k):
        return lined(xall, p * xshare + k * xpiece, xpiece)
    def xsection(k):
        return lined(xall, k * xshare, xshare)
    xcore, xscatter, xgather, xcopy = pair(), pair(), pair(), pair()

    def scatter():
        return exchange(
            team, seat, member, lambda d: lined(xpart, d * xpiece, xpiece), lambda k: xgot2.at[k],
            xgot2.at[pl.ds(0, team - 1)], *xscatter,
        )

    def turned(columns):
        depth = columns.stop
        oext[columns.start // half, size:bottom, :] = dot(wext[size:bottom, :depth], rinv[:depth, columns]).astype(bf16)

    def imaged(q):
        def keep(i, z):
            zext[q, i * size:(i + 1) * size, :] = z

        applied(oext.at[q], 1, range(count), slice(None), keep)

    def cross_half():
        crossed = wext.at[pl.ds(size, body), theirs]
        remote(crossed, crossed, osem, orecv, cols=other).wait_recv()
        gx[...] = inner(wext[size:bottom, :half], wext[size:bottom, half:])
        for j in range(across):
            xpack[j * half:(j + 1) * half, :] = gx[:, j * LANES:(j + 1) * LANES]
        if xpack.shape[0] > across * half:
            xpack[across * half:, :] = jnp.zeros((xpack.shape[0] - across * half, LANES), f32)
        finish = exchange(
            h, p, mate, lambda d: lined(xpack, d * xshare, xshare), lambda k: xgot1.at[k],
            xgot1.at[pl.ds(0, h - 1)], *xcore
        )
        xgot1[p] = xpack[pl.ds(pl.multiple_of(p * xshare, 8), xshare), :]
        finish()
        xpart[...] = summed(xgot1, h)
        scatter()
        pl.when(flat < last)(lambda: halo(0, 0).start())
        pl.when(flat > 0)(lambda: halo(1, 0).start())

    def join():
        pl.when(y == 0)(opposite)
        arrived = xgot2.at[pl.ds(0, team - 1)]
        remote(arrived, arrived, *xscatter, **member(lax.rem(seat + 1, team))).wait()
        xgot2[seat] = xpart[pl.ds(pl.multiple_of(seat * xpiece, 8), xpiece), :]
        xall[pl.ds(pl.multiple_of(p * xshare + seat * xpiece, 8), xpiece), :] = summed(xgot2, team)
        exchange(team, seat, member, lambda d: xspot(seat), lambda k: xspot(seat), arrived, *xgather)
        pl.when(flat < last)(lambda: halo(0, 1).start())
        pl.when(flat > 0)(lambda: halo(1, 1).start())

        @pl.when(y == 0)
        def _():
            for n in early:
                further(n).start()

    def rest():
        linv0[...] = linv1[...]
        rinv[:half, :half] = linv0[...].T.astype(bf16)
        turned(slice(0, half))

        def early_image():
            pl.when(flat > 0)(lambda: halo(0, 0).wait_recv())
            pl.when(flat < last)(lambda: halo(1, 0).wait_recv())
            oext[0, :size, :] = dot(wext[:size, :half], rinv[:half, :half]).astype(bf16)
            oext[0, bottom:, :] = dot(wext[bottom:, :half], rinv[:half, :half]).astype(bf16)
            imaged(0)
            total[:half, :half] = inner(oext[0, size:bottom, :], zext[0])

        pl.when(y == 0)(early_image)
        arrived = xgot2.at[pl.ds(0, team - 1)]
        remote(arrived, arrived, *xgather, **member(lax.rem(seat + 1, team))).wait()
        finish = exchange(
            h, p, mate, lambda d: xsection(p), lambda k: xsection(p), lined(xall, 0, (h - 1) * xshare), *xcopy
        )
        pl.when(y == 1)(early_image)
        finish()
        for j in range(across):
            gx[:, j * LANES:(j + 1) * LANES] = xall[j * half:(j + 1) * half, :]
        tall[...] = fine(linv0[...], gx[...])
        load(1)
        for i in range(across):
            cwork[i, :, i * LANES:] = cwork[i, :, i * LANES:] - fine(
                tall[:, i * LANES:(i + 1) * LANES], tall[:, i * LANES:], ((0,), (0,))
            )
        gx[...] = fine(tall[...], linv0[...], ((0,), (0,)))

    pl.when(y == 0)(lambda: load(0))

    def factor_step(g, carry):
        @pl.when((g == 0) & (y == 1))
        def _():
            cross_half()
            opposite()
            load(0)

        eliminate(cwork, lax.rem(g, across), linv1, cpanel, hold)
        pl.when((g == 0) & (y == 0))(cross_half)
        pl.when(((g == 0) & (y == 1)) | ((g == across - 1) & (y == 0)))(join)
        pl.when(g == across - 1)(rest)
        return carry

    lax.fori_loop(0, 2 * across, factor_step, 0)
    rinv[half:, half:] = linv1[...].T.astype(bf16)
    rinv[:half, half:] = (-fine(gx[...], linv1[...], ((0,), (1,)))).astype(bf16)
    pl.when(flat > 0)(lambda: halo(0, 1).wait_recv())
    pl.when(flat < last)(lambda: halo(1, 1).wait_recv())
    oext[1] = dot(wext[...], rinv[:, half:]).astype(bf16)
    pl.when(y == 0)(lambda: send_late(late[:1]))
    imaged(1)
    total[:half, half:] = inner(oext[0, size:bottom, :], zext[1])
    def place(j, source, first, k):
        return source.at[pl.ds(first, body), k], ortho.at[pl.ds(pl.multiple_of((c if j else other) * body, size), body), :]

    def settle(j):
        source, first = (oext.at[y], size) if j else (home, 0)

        def col(k):
            return lanes(k, width)

        own_copy = pltpu.make_async_copy(*place(j, source, first, col(p)), isem.at[j])
        own_copy.start()
        for step in range(1, h):
            k = lax.rem(p + step, h)
            src_ref, dst_ref = place(j, source, first, col(k))
            remote(src_ref, dst_ref, msend.at[j], mrecv.at[j], **mate(k)).start()

        def finish():
            own_copy.wait()
            if h > 1:
                moved = ortho.at[pl.ds(0, (h - 1) * body), :]
                remote(moved, moved, msend.at[j], mrecv.at[j], **mate(lax.rem(p + 1, h))).wait()

        return finish

    parts = psum.shape[0]
    rows_of = order // parts
    lump = rows_of // nr
    sends = [pair() for _ in range(4)]

    def band(n):
        return slice(n * rows_of, (n + 1) * rows_of)

    def share_of(n):
        for k in range(2):
            for q in range(h):
                ppack[n, q, k] = total[band(n), (k * h + q) * width:(k * h + q + 1) * width].astype(bf16)
        s, v = sends[0]
        return exchange(
            h, p, mate, lambda d: ppack.at[n, d], lambda k: pgot1.at[n, k], pgot1.at[n, pl.ds(0, h - 1)], s.at[n], v.at[n]
        )

    def crossing(n):
        s, v = sends[1]
        return remote(phalf.at[n, 0], phalf.at[n, 1], s.at[n], v.at[n], cols=other)

    def joined(n, k):
        mine_here = total[band(n), lanes(k * h + p, width)]
        for step in range(1, h):
            mine_here = mine_here + pgot1[n, lax.rem(p + step, h), k].astype(f32)
        return mine_here

    def launch(n):
        phalf[n, 0] = joined(n, 1 - y).astype(bf16)
        crossing(n).start()

    def spot(n, k):
        return psum.at[n, pl.ds(pl.multiple_of(k * lump, lump), lump), :]

    def scattered(n):
        crossing(n).wait()
        psum[n] = (joined(n, y) + phalf[n, 1].astype(f32)).astype(bf16)
        s, v = sends[2]
        done = exchange(
            nr, r, line, lambda d: spot(n, d), lambda k: pgot2.at[n, k], pgot2.at[n, pl.ds(0, nr - 1)], s.at[n], v.at[n]
        )
        pgot2[n, r] = psum[n, pl.ds(pl.multiple_of(r * lump, lump), lump), :]
        return done

    def gathered(n):
        def place_of(k):
            return pall.at[n, pl.ds(pl.multiple_of(k * lump, lump), lump), :]

        pall[n, pl.ds(pl.multiple_of(r * lump, lump), lump), :] = sum(
            (pgot2[n, k].astype(f32) for k in range(1, nr)), pgot2[n, 0].astype(f32)
        ).astype(bf16)
        s, v = sends[3]
        return exchange(nr, r, line, lambda d: place_of(r), lambda k: place_of(r), pgot2.at[n, pl.ds(0, nr - 1)], s.at[n], v.at[n])

    shared = [share_of(n) for n in range(parts // 2)]
    total[half:, :half] = inner(oext[1, size:bottom, :], zext[0])
    total[half:, half:] = inner(oext[1, size:bottom, :], zext[1])
    for n in range(parts // 2):
        shared[n]()
        launch(n)
    shared = [share_of(n) for n in range(parts // 2, parts)]
    for n in range(parts // 2, parts):
        shared[n - parts // 2]()
        launch(n)
    pl.when(y == 0)(lambda: send_late(late[1:]))
    finish_own = settle(1)

    @pl.when(y == 0)
    def _():
        for i in range(count):
            rows = slice(i * size, (i + 1) * size)
            home[rows, :] = dot(wsend[rows, :], rinv[:half, :half]).astype(bf16)

    spread_out = [scattered(n) for n in range(parts)]

    @pl.when(y == 1)
    def _():
        all_further(0).wait_recv()
        for i in (i for n in early for i in range(chunks[n][0], sum(chunks[n]))):
            rows = slice(i * size, (i + 1) * size)
            home[rows, :] = (dot(far[rows, :], rinv[:half, half:]) + dot(wsend[rows, :], rinv[half:, half:])).astype(bf16)

    brought = []
    for n in range(parts):
        spread_out[n]()
        brought.append(gathered(n))

    @pl.when(y == 1)
    def _():
        all_further(1).wait_recv()

    finish_other = settle(0)
    for n in range(parts):
        brought[n]()
        projected[band(n), :] = pall[n].astype(f32)

    finish_own()
    finish_other()

    @pl.when(y == 0)
    def _():
        all_further(0).wait_send()
        all_further(1).wait_send()

    for q in range(2):
        pl.when(flat < last)(lambda: halo(0, q).wait_send())
        pl.when(flat > 0)(lambda: halo(1, q).wait_send())
    remote(wsend, wsend, osem, orecv, cols=other).wait_send()
    over.wait_send()
    pl.when(r < nr - 1)(lambda: down().wait_send())
    pl.when(r > 0)(lambda: up().wait_send())
    for j in (0, 1):
        for s in range(3):
            each(j, s, lambda step: to_mate(j, s, step).wait_send())


def shards(nr, nc, basis, lower, diag, upper, inverse):
    blocks, size, _ = diag.shape
    width = basis.shape[1]
    h = nc // 2
    half = width * h
    order = 2 * half
    count = blocks // nc
    across = half // LANES
    body = count * size
    f32, bf16 = jnp.float32, jnp.bfloat16

    def parcel(lines, parts):
        piece = -(-lines // (h * parts * 8)) * 8
        return piece * parts, piece

    share, piece = parcel(across * (across + 1) // 2 * LANES, nr)
    xshare, xpiece = parcel(across * half, 2 * nr)
    parts = 4 if order // nr >= 8 * SUB else 1
    rows_of = order // parts
    dma = pltpu.SemaphoreType.DMA
    bext = (2, (count + 2) * size, half)
    ext = ((count + 2) * size, order)
    chunks = (count - 4) // 2 + 4
    square = pltpu.VMEM((half, half), f32)
    opflops = 16 * count * size * size * order + 6 * count * size * order * order
    return pl.pallas_call(
        functools.partial(whole_kernel, nr, nc),
        out_shape=(pltpu.VMEM(basis.shape, bf16), pltpu.VMEM((order, width), f32)),
        in_specs=[ANY] * 5,
        out_specs=(VMEM, VMEM),
        scratch_shapes=[
            pltpu.VMEM(bext, bf16), pltpu.VMEM(ext, bf16), pltpu.VMEM((body, half), bf16), pltpu.VMEM(bext, bf16),
            pltpu.VMEM((2, 4, count, size, size), bf16),
            square, square, pltpu.VMEM((order, order), f32), pltpu.VMEM((order, order), bf16),
            pltpu.VMEM((across, LANES, half), f32), pltpu.VMEM((LANES, LANES), f32), pltpu.VMEM((2, SUB, SUB, LANES), f32),
            square, square, square,
            pltpu.VMEM((h * share, LANES), f32), pltpu.VMEM((h, share, LANES), f32), pltpu.VMEM((share, LANES), f32),
            pltpu.VMEM((nr, piece, LANES), f32), pltpu.VMEM((2, h * share, LANES), f32),
            pltpu.VMEM((h * xshare, LANES), f32), pltpu.VMEM((h, xshare, LANES), f32), pltpu.VMEM((xshare, LANES), f32),
            pltpu.VMEM((2 * nr, xpiece, LANES), f32), pltpu.VMEM((h * xshare, LANES), f32),
            pltpu.VMEM((parts, h, 2, rows_of, width), bf16), pltpu.VMEM((parts, 2, rows_of, width), bf16),
            pltpu.VMEM((parts, nr, rows_of // nr, width), bf16), pltpu.VMEM((parts, rows_of, width), bf16),
            pltpu.VMEM((parts, h, 2, rows_of, width), bf16), pltpu.VMEM((parts, rows_of, width), bf16),
            pltpu.VMEM((body, half), bf16), pltpu.VMEM((body, half), bf16), pltpu.VMEM((2, body, half), bf16),
            pltpu.VMEM((2, body, half), bf16),
            pltpu.SemaphoreType.REGULAR((rounds(nr, nc) - 1,)),
            dma((2,)), dma((2, 3)), dma((2, 3)), dma((2,)),
            dma, dma, dma((2, 2)), dma((2, 2)), dma((2,)), dma((2,)),
            dma((2,)), dma((2,)), dma((2,)),
        ] + [dma] * 20 + [dma((parts,))] * 8,
        compiler_params=pltpu.CompilerParams(has_side_effects=True, collective_id=1),
        cost_estimate=pl.CostEstimate(flops=opflops, bytes_accessed=1 << 24, transcendentals=0),
        name="krylov",
    )(basis, lower, diag, upper, inverse)


def solution(mesh):
    in_specs = (
        P("rows", "cols"),
        P("rows", None, None),
        P("rows", None, None),
        P("rows", None, None),
        P("rows", None, None),
    )
    out_specs = (P("rows", "cols"), P(None, "cols"))
    body = functools.partial(shards, mesh.shape["rows"], mesh.shape["cols"])
    return jax.shard_map(body, mesh=mesh, in_specs=in_specs, out_specs=out_specs, check_vma=False)
```

```python
import functools

import jax
import jax.numpy as jnp
from jax import lax
from jax.experimental import pallas as pl
from jax.experimental.pallas import tpu as pltpu
from jax.sharding import PartitionSpec as P

LANES = 128
MESH = pl.DeviceIdType.MESH
VMEM = pl.BlockSpec(memory_space=pltpu.VMEM)
ANY = pl.BlockSpec(memory_space=pl.ANY)
SUB = 8
HI = lax.Precision.HIGHEST

def factor_tile(block, hold):
    size = block.shape[0]
    wide = (SUB, size)
    tiles = size // SUB
    row_of = lax.broadcasted_iota(jnp.int32, wide, 0)
    lane_of = lax.broadcasted_iota(jnp.int32, wide, 1)
    a = [block[t * SUB:(t + 1) * SUB, :] for t in range(tiles)]
    out = []
    for t in range(tiles):
        base = t * SUB
        at = a[t]
        last = t == tiles - 1
        inside = (lane_of >= base) & (lane_of < base + SUB)
        unity = jnp.where(lane_of == row_of + base, 1.0, 0.0).astype(jnp.float32)
        mixed = jnp.where(inside, unity, at)
        pivot = {}
        for j in range(SUB):
            hold[t % 2, j] = jnp.broadcast_to(at[:, base + j:base + j + 1], wide)
        for j in range(SUB):
            for i in range(j, SUB):
                pivot[i, j] = hold[t % 2, j, pl.ds(i, SUB, stride=0), :]
        rows = [jnp.broadcast_to(mixed[i:i + 1, :], wide) for i in range(SUB)]
        unit = {}
        solved = [None] * SUB
        if not last:
            ahead = jnp.where(inside, 0.0, a[t + 1])
            edge = [jnp.broadcast_to(a[t + 1][:, base + j:base + j + 1], wide) for j in range(SUB)]
        fin = jnp.zeros(wide, jnp.float32)
        for j in range(SUB):
            d = pivot[j, j]
            root = lax.rsqrt(d)
            inv = 1.0 / d
            for i in range(j + 1, SUB):
                unit[i, j] = pivot[i, j] * inv
            for i in range(j + 1, SUB):
                for q in range(j + 1, i + 1):
                    pivot[i, q] = pivot[i, q] - unit[i, j] * pivot[q, j]
            for i in range(j + 1, SUB):
                rows[i] = rows[i] - unit[i, j] * rows[j]
            fin = jnp.where(row_of == j, rows[j] * root, fin)
            if not last:
                solved[j] = rows[j] * inv
                ahead = ahead - edge[j] * solved[j]
                for q in range(j + 1, SUB):
                    edge[q] = edge[q] - edge[j] * unit[q, j]
        out.append(jnp.where(lane_of < base + SUB, fin, 0.0))
        if last:
            break
        a[t + 1] = ahead
        if t + 2 < tiles:
            for j in range(SUB - 1, -1, -1):
                for i in range(j):
                    solved[i] = solved[i] - unit[j, i] * solved[j]
        for s in range(t + 2, tiles):
            new = jnp.where(inside, 0.0, a[s])
            for j in range(SUB - 1, -1, -1):
                c = jnp.broadcast_to(a[s][:, base + j:base + j + 1], wide)
                new = new - c * solved[j]
            a[s] = new
    return jnp.concatenate(out, axis=0)


def eliminate(work_ref, b, out_ref, panel_ref, hold_ref):
    n, size, _ = work_ref.shape
    at = [work_ref[b, :, i * size:(i + 1) * size] for i in range(n)]
    block = at[0]
    for i in range(1, n):
        block = jnp.where(b == i, at[i], block)
    panel_ref[...] = factor_tile(block, hold_ref)

    def stage(k):
        linv = panel_ref[...]
        rows = slice(k * size, (k + 1) * size)
        if k:
            out_ref[rows, :k * size] = fine(linv, out_ref[rows, :k * size])
        out_ref[rows, rows] = linv
        if k + 1 < n:
            out_ref[rows, (k + 1) * size:] = jnp.zeros((size, (n - k - 1) * size), jnp.float32)
            right = fine(linv, work_ref[k, :, (k + 1) * size:n * size])
            known = jnp.concatenate([right, out_ref[rows, :(k + 1) * size]], axis=1)
            for i in range(k + 1, n):
                step = fine(right[:, (i - k - 1) * size:(i - k) * size], known, ((0,), (0,)))
                lines = slice(i * size, (i + 1) * size)
                cut = (n - k - 1) * size
                work_ref[i, :, (k + 1) * size:n * size] = work_ref[i, :, (k + 1) * size:n * size] - step[:, :cut]
                if k:
                    out_ref[lines, :k * size] = out_ref[lines, :k * size] - step[:, cut:cut + k * size]
                out_ref[lines, rows] = -step[:, cut + k * size:]

    for k in range(n):
        pl.when(b == k)(functools.partial(stage, k))


def dot(left, right):
    return jnp.dot(left, right, preferred_element_type=jnp.float32)


def inner(left, right):
    return lax.dot_general(
        left, right, (((0,), (0,)), ((), ())), preferred_element_type=jnp.float32
    )


def fine(left, right, dims=((1,), (0,))):
    return lax.dot_general(
        left, right, (dims, ((), ())), precision=HI, preferred_element_type=jnp.float32
    )


def remote(src, dst, send, recv, **where):
    return pltpu.make_async_remote_copy(
        src_ref=src, dst_ref=dst, send_sem=send, recv_sem=recv, device_id=where, device_id_type=MESH
    )


def exchange(count, me, where, source, target, whole, send, recv):
    for step in range(1, count):
        peer = lax.rem(me + step, count)
        remote(source(peer), target(me), send, recv, **where(peer)).start()

    def finish():
        if count > 1:
            remote(whole, whole, send, recv, **where(lax.rem(me + 1, count))).wait()

    return finish


def around(nr, nc, r, c):
    h = nc // 2
    for step in range(1, nc):
        yield True, r, lax.rem(c + step, nc)
    for by in (1, -1):
        there = (r + by >= 0) & (r + by < nr)
        for k in range(h):
            yield there, r + by, (c // h) * h + k
    for by in (2, -2):
        yield (r + by >= 0) & (r + by < nr), r + by, c


def rounds(nr, nc):
    h = nc // 2
    seen, edge, far = {(0, 0)}, {(0, 0)}, 0
    while len(seen) < nr * nc:
        new = set()
        for r, c in edge:
            new |= {(r, k) for k in range(nc)}
            new |= {(r + by, c // h * h + k) for by in (1, -1) for k in range(h)}
            new |= {(r + by, c) for by in (2, -2)}
        edge = {d for d in new if 0 <= d[0] < nr} - seen
        seen |= edge
        far += 1
    return far


def tell(sem, nr, nc, r, c):
    for there, row, col in around(nr, nc, r, c):
        def signal():
            pl.semaphore_signal(sem, inc=1, device_id=dict(rows=row, cols=col), device_id_type=MESH)

        if there is True:
            signal()
        else:
            pl.when(there)(signal)


def hear(sem, nr, nc, r, c):
    pl.semaphore_wait(sem, sum(1 if t is True else t.astype(jnp.int32) for t, _, _ in around(nr, nc, r, c)))


def lined(ref, start, extent):
    return ref.at[pl.ds(pl.multiple_of(start, 8), extent), :]


def summed(ref, count):
    return sum((ref[k] for k in range(1, count)), ref[0])


def whole_kernel(
    nr, nc, basis, lower, diag, upper, inverse, ortho, projected,
    bext, wext, wsend, oext, held, gy, gx, total, rinv, cwork, cpanel, hold, linv0, linv1, tall,
    ypack, ygot1, ypart, ygot2, yall, xpack, xgot1, xpart, xgot2, xall,
    pgot1, phalf, pgot2, psum, ppack, pall,
    far, home, zext, mix,
    known, wsem, bsend, brecv, esem, osem, orecv, hsend, hrecv, fsend, frecv, isem, msend, mrecv, *sems,
):
    sems = list(sems)

    def pair():
        return sems.pop(0), sems.pop(0)

    bf16, f32 = jnp.bfloat16, jnp.float32
    r, c = lax.axis_index("rows"), lax.axis_index("cols")
    h = nc // 2
    y, p = c // h, lax.rem(c, h)
    other = (1 - y) * h + p
    _, _, count, size, _ = held.shape
    width = basis.shape[1]
    half = width * h
    order = 2 * half
    body = count * size
    bottom = size + body
    team = 2 * nr
    seat = 2 * r + y

    def mate(k):
        return dict(cols=y * h + k)

    def member(k):
        return dict(rows=k // 2, cols=lax.rem(k, 2) * h + p)

    def line(k):
        return dict(rows=k)

    def at(i):
        return pl.ds(pl.multiple_of(i * size, size), size)

    def lanes(k, extent):
        return pl.ds(pl.multiple_of(k * extent, LANES), extent)

    wl, wd, wu, wi = (held.at[:, k] for k in range(4))
    for j, g in enumerate((other, c)):
        for k, part in enumerate((lower, diag, upper, inverse)):
            pltpu.make_async_copy(part.at[pl.ds(g * count, count)], held.at[j, k], wsem.at[j]).start()

    def weighed(j):
        pltpu.make_async_copy(held.at[1 - j], held.at[j], wsem.at[j]).wait()

    spans = [(0, size), (size, 3 * size), (bottom, size), (4 * size, body - 3 * size)]

    def group(j, k):
        return y * h + k if j else (1 - y) * h + k

    def leaving(j, s, k):
        start, extent = spans[s]
        return basis.at[pl.ds(pl.multiple_of(group(j, k) * body - size + start, size), extent), :]

    def landing(j, s, k):
        start, extent = spans[s]
        return bext.at[j, pl.ds(start, extent), lanes(k, width)]

    def within(s, g, action):
        if s == 0:
            pl.when(g > 0)(action)
        elif s == 2:
            pl.when(g < nc - 1)(action)
        else:
            action()

    def own(j, s):
        return pltpu.make_async_copy(leaving(j, s, p), landing(j, s, p), brecv.at[j, s])

    def to_mate(j, s, step):
        k = lax.rem(p + step, h)
        return remote(leaving(j, s, k), landing(j, s, p), bsend.at[j, s], brecv.at[j, s], **mate(k))

    def down():
        return remote(
            basis.at[pl.ds(nc * body - size, size), :], landing(1 - y, 0, p), esem.at[0],
            brecv.at[1 - y, 0], rows=r + 1, cols=y * h,
        )

    def up():
        return remote(
            basis.at[pl.ds(0, size), :], landing(y, 2, p), esem.at[1],
            brecv.at[y, 2], rows=r - 1, cols=y * h + h - 1,
        )

    for j in (0, 1):
        for s in (1, 3, 0, 2):
            within(s, group(j, p), lambda: own(j, s).start())

    barrier = pltpu.get_barrier_semaphore()
    tell(barrier, nr, nc, r, c)
    hear(barrier, nr, nc, r, c)
    heard = known.shape[0]
    tell(known.at[0], nr, nc, r, c)
    told = [0]

    def spread():
        if told[0] < heard:
            hear(known.at[told[0]], nr, nc, r, c)
            told[0] += 1
            if told[0] < heard:
                tell(known.at[told[0]], nr, nc, r, c)

    def each(j, s, action):
        for step in range(1, h):
            k = lax.rem(p + step, h)
            within(s, group(j, k), functools.partial(action, step))

    for s in (1, 3):
        for step in range(1, h):
            to_mate(0, s, step).start()
    pl.when(r < nr - 1)(lambda: down().start())
    pl.when(r > 0)(lambda: up().start())
    for j, s in ((0, 0), (0, 2), (1, 1), (1, 3), (1, 0), (1, 2)):
        each(j, s, lambda step: to_mate(j, s, step).start())

    for j in (0, 1):
        @pl.when((r == 0) & (group(j, p) == 0))
        def _():
            bext[j, 0:size, :] = jnp.zeros((size, half), bf16)

        @pl.when((r == nr - 1) & (group(j, p) == nc - 1))
        def _():
            bext[j, bottom:bottom + size, :] = jnp.zeros((size, half), bf16)

    @pl.when((r == 0) & (c == 0))
    def _():
        wext[0:size, :] = jnp.zeros((size, order), bf16)

    @pl.when((r == nr - 1) & (c == nc - 1))
    def _():
        wext[bottom:bottom + size, :] = jnp.zeros((size, order), bf16)

    def arrive(j, s):
        g = group(j, p)
        start, extent = spans[s]
        full = bext.at[j, pl.ds(start, extent), :]
        comes = {0: (g > 0) | (r > 0), 2: (g < nc - 1) | (r < nr - 1)}.get(s, r >= 0)
        pl.when(comes)(lambda: pltpu.make_async_copy(bext.at[1 - j, pl.ds(start, extent), :], full, brecv.at[j, s]).wait())

    def applied(field, j, some, columns, out):
        for i in some:
            mixed = (
                dot(wl[j, i], field[i * size:(i + 1) * size, columns])
                + dot(wd[j, i], field[(i + 1) * size:(i + 2) * size, columns])
                + dot(wu[j, i], field[(i + 2) * size:(i + 3) * size, columns])
            )
            mix[j, i * size:(i + 1) * size, :] = mixed.astype(bf16)
        for i in some:
            out(i, dot(wi[j, i], mix[j, i * size:(i + 1) * size, :]).astype(bf16))

    mine = lanes(y, half)
    chunks = [(1, 1), (2, 1)] + [(i, 2) for i in range(3, count - 1, 2)] + [(0, 1), (count - 1, 1)]

    def cross(n, to=None):
        start, extent = chunks[n][0] * size, chunks[n][1] * size
        return remote(
            wsend.at[pl.ds(start, extent), :],
            wext.at[pl.ds(size + start, extent), mine if to is None else to],
            osem, orecv, cols=other,
        )

    weighed(0)
    arrive(0, 1)

    def first(some):
        def keep(i, w):
            wsend[i * size:(i + 1) * size, :] = w

        applied(bext.at[0], 0, some, slice(None), keep)

    def second(some):
        def keep(i, w):
            wext[(i + 1) * size:(i + 2) * size, mine] = w

        applied(bext.at[1], 1, some, slice(None), keep)

    for n in range(len(chunks) - 2):
        start, extent = chunks[n]
        if n == 1:
            arrive(0, 3)
        first(range(start, start + extent))
        cross(n).start()
        if n == 1:
            spread()
    weighed(1)
    arrive(1, 1)
    arrive(1, 3)
    second(range(1, count - 1))
    spread()
    mid = slice(size, body - size)
    gy[...] = inner(wsend[mid, :], wsend[mid, :])
    spread()
    own_half = wext[2 * size:body, mine]
    gy[...] += inner(own_half, own_half)
    arrive(0, 0)
    arrive(0, 2)
    first((0, count - 1))
    for n in range(len(chunks) - 2, len(chunks)):
        cross(n).start()
    spread()
    arrive(1, 0)
    arrive(1, 2)
    second((0, count - 1))
    for _ in range(heard):
        spread()
    for rows in (slice(0, size), slice(body - size, body)):
        own_half = wext[rows.start + size:rows.stop + size, mine]
        gy[...] += inner(wsend[rows, :], wsend[rows, :]) + inner(own_half, own_half)

    early = list(range(len(chunks) // 2))
    late = sorted(range(len(chunks) // 2, len(chunks)), key=lambda n: chunks[n][1])

    def further(n):
        start, extent = chunks[n][0] * size, chunks[n][1] * size
        if n in early:
            source, target = wext.at[pl.ds(size + start, extent), :half], far.at[pl.ds(start, extent), :]
        else:
            source, target = oext.at[1, pl.ds(size + start, extent), :], home.at[pl.ds(start, extent), :]
        return remote(source, target, fsend.at[int(n in late)], frecv.at[int(n in late)], cols=other)

    def all_further(kind):
        some = (early, late)[kind]
        extent = sum(chunks[n][1] for n in some) * size
        part = far.at[pl.ds(0, extent), :]
        return remote(part, part, fsend.at[kind], frecv.at[kind], cols=other)

    def send_late(some):
        for n in some:
            further(n).start()

    across = half // LANES
    place = 0
    for i in range(across):
        for j in range(i, across):
            ypack[place * LANES:(place + 1) * LANES, :] = gy[
                i * LANES:(i + 1) * LANES, j * LANES:(j + 1) * LANES
            ]
            place += 1
    if ypack.shape[0] > place * LANES:
        ypack[place * LANES:, :] = jnp.zeros((ypack.shape[0] - place * LANES, LANES), f32)
    share, piece = ygot1.shape[1], ygot2.shape[1]
    s, v = pair()
    finish = exchange(
        h, p, mate, lambda d: lined(ypack, d * share, share), lambda k: ygot1.at[k],
        ygot1.at[pl.ds(0, h - 1)], s, v
    )
    ygot1[p] = ypack[pl.ds(pl.multiple_of(p * share, 8), share), :]
    finish()
    ypart[...] = summed(ygot1, h)
    s, v = pair()
    finish = exchange(
        nr, r, line, lambda d: lined(ypart, d * piece, piece), lambda k: ygot2.at[k],
        ygot2.at[pl.ds(0, nr - 1)], s, v
    )
    ygot2[r] = ypart[pl.ds(pl.multiple_of(r * piece, 8), piece), :]
    finish()

    def yspot(k):
        return yall.at[y, pl.ds(pl.multiple_of(p * share + k * piece, 8), piece), :]

    def yshare(side, k):
        return yall.at[side, pl.ds(pl.multiple_of(k * share, 8), share), :]

    yall[y, pl.ds(pl.multiple_of(p * share + r * piece, 8), piece), :] = summed(ygot2, nr)
    s, v = pair()
    exchange(nr, r, line, lambda d: yspot(r), lambda k: yspot(r), ygot2.at[pl.ds(0, nr - 1)], s, v)()
    s, v = pair()
    over = remote(yshare(y, p), yshare(y, p), s, v, cols=other)
    over.start()

    def both(side, sems_of):
        rest = yall.at[side, pl.ds(0, (h - 1) * share), :]
        exchange(h, p, mate, lambda d: yshare(side, p), lambda k: yshare(side, p), rest, *sems_of)()

    both(y, pair())
    opposite_sems = pair()

    def opposite():
        over.wait_recv()
        both(1 - y, opposite_sems)

    def load(which):
        place = 0
        for i in range(across):
            for j in range(i, across):
                cwork[i, :, j * LANES:(j + 1) * LANES] = yall[which, place * LANES:(place + 1) * LANES, :]
                place += 1

    flat = r * nc + c
    last = nr * nc - 1

    def halo(kind, q):
        start = (body, size)[kind]
        target = (0, bottom)[kind]
        to = flat + (1, -1)[kind]
        part = pl.ds(q * half, half)
        return remote(
            wext.at[pl.ds(start, size), part], wext.at[pl.ds(target, size), part], hsend.at[kind, q],
            hrecv.at[kind, q], rows=to // nc, cols=lax.rem(to, nc),
        )


    theirs = lanes(1 - y, half)
    xshare, xpiece = xgot1.shape[1], xgot2.shape[1]
    def xspot(k):
        return lined(xall, p * xshare + k * xpiece, xpiece)
    def xsection(k):
        return lined(xall, k * xshare, xshare)
    xcore, xscatter, xgather, xcopy = pair(), pair(), pair(), pair()

    def scatter():
        return exchange(
            team, seat, member, lambda d: lined(xpart, d * xpiece, xpiece), lambda k: xgot2.at[k],
            xgot2.at[pl.ds(0, team - 1)], *xscatter,
        )

    def turned(columns):
        depth = columns.stop
        oext[columns.start // half, size:bottom, :] = dot(wext[size:bottom, :depth], rinv[:depth, columns]).astype(bf16)

    def imaged(q):
        def keep(i, z):
            zext[q, i * size:(i + 1) * size, :] = z

        applied(oext.at[q], 1, range(count), slice(None), keep)

    def cross_half():
        crossed = wext.at[pl.ds(size, body), theirs]
        remote(crossed, crossed, osem, orecv, cols=other).wait_recv()
        gx[...] = inner(wext[size:bottom, :half], wext[size:bottom, half:])
        for j in range(across):
            xpack[j * half:(j + 1) * half, :] = gx[:, j * LANES:(j + 1) * LANES]
        if xpack.shape[0] > across * half:
            xpack[across * half:, :] = jnp.zeros((xpack.shape[0] - across * half, LANES), f32)
        finish = exchange(
            h, p, mate, lambda d: lined(xpack, d * xshare, xshare), lambda k: xgot1.at[k],
            xgot1.at[pl.ds(0, h - 1)], *xcore
        )
        xgot1[p] = xpack[pl.ds(pl.multiple_of(p * xshare, 8), xshare), :]
        finish()
        xpart[...] = summed(xgot1, h)
        scatter()
        pl.when(flat < last)(lambda: halo(0, 0).start())
        pl.when(flat > 0)(lambda: halo(1, 0).start())

    def join():
        pl.when(y == 0)(opposite)
        arrived = xgot2.at[pl.ds(0, team - 1)]
        remote(arrived, arrived, *xscatter, **member(lax.rem(seat + 1, team))).wait()
        xgot2[seat] = xpart[pl.ds(pl.multiple_of(seat * xpiece, 8), xpiece), :]
        xall[pl.ds(pl.multiple_of(p * xshare + seat * xpiece, 8), xpiece), :] = summed(xgot2, team)
        exchange(team, seat, member, lambda d: xspot(seat), lambda k: xspot(seat), arrived, *xgather)
        pl.when(flat < last)(lambda: halo(0, 1).start())
        pl.when(flat > 0)(lambda: halo(1, 1).start())

        @pl.when(y == 0)
        def _():
            for n in early:
                further(n).start()

    def rest():
        linv0[...] = linv1[...]
        rinv[:half, :half] = linv0[...].T.astype(bf16)
        turned(slice(0, half))

        def early_image():
            pl.when(flat > 0)(lambda: halo(0, 0).wait_recv())
            pl.when(flat < last)(lambda: halo(1, 0).wait_recv())
            oext[0, :size, :] = dot(wext[:size, :half], rinv[:half, :half]).astype(bf16)
            oext[0, bottom:, :] = dot(wext[bottom:, :half], rinv[:half, :half]).astype(bf16)
            imaged(0)
            total[:half, :half] = inner(oext[0, size:bottom, :], zext[0])

        pl.when(y == 0)(early_image)
        arrived = xgot2.at[pl.ds(0, team - 1)]
        remote(arrived, arrived, *xgather, **member(lax.rem(seat + 1, team))).wait()
        finish = exchange(
            h, p, mate, lambda d: xsection(p), lambda k: xsection(p), lined(xall, 0, (h - 1) * xshare), *xcopy
        )
        pl.when(y == 1)(early_image)
        finish()
        for j in range(across):
            gx[:, j * LANES:(j + 1) * LANES] = xall[j * half:(j + 1) * half, :]
        tall[...] = fine(linv0[...], gx[...])
        load(1)
        for i in range(across):
            cwork[i, :, i * LANES:] = cwork[i, :, i * LANES:] - fine(
                tall[:, i * LANES:(i + 1) * LANES], tall[:, i * LANES:], ((0,), (0,))
            )
        gx[...] = fine(tall[...], linv0[...], ((0,), (0,)))

    pl.when(y == 0)(lambda: load(0))

    def factor_step(g, carry):
        @pl.when((g == 0) & (y == 1))
        def _():
            cross_half()
            opposite()
            load(0)

        eliminate(cwork, lax.rem(g, across), linv1, cpanel, hold)
        pl.when((g == 0) & (y == 0))(cross_half)
        pl.when(((g == 0) & (y == 1)) | ((g == across - 1) & (y == 0)))(join)
        pl.when(g == across - 1)(rest)
        return carry

    lax.fori_loop(0, 2 * across, factor_step, 0)
    rinv[half:, half:] = linv1[...].T.astype(bf16)
    rinv[:half, half:] = (-fine(gx[...], linv1[...], ((0,), (1,)))).astype(bf16)
    pl.when(flat > 0)(lambda: halo(0, 1).wait_recv())
    pl.when(flat < last)(lambda: halo(1, 1).wait_recv())
    oext[1] = dot(wext[...], rinv[:, half:]).astype(bf16)
    pl.when(y == 0)(lambda: send_late(late[:1]))
    imaged(1)
    total[:half, half:] = inner(oext[0, size:bottom, :], zext[1])
    def place(j, source, first, k):
        return source.at[pl.ds(first, body), k], ortho.at[pl.ds(pl.multiple_of((c if j else other) * body, size), body), :]

    def settle(j):
        source, first = (oext.at[y], size) if j else (home, 0)

        def col(k):
            return lanes(k, width)

        own_copy = pltpu.make_async_copy(*place(j, source, first, col(p)), isem.at[j])
        own_copy.start()
        for step in range(1, h):
            k = lax.rem(p + step, h)
            src_ref, dst_ref = place(j, source, first, col(k))
            remote(src_ref, dst_ref, msend.at[j], mrecv.at[j], **mate(k)).start()

        def finish():
            own_copy.wait()
            if h > 1:
                moved = ortho.at[pl.ds(0, (h - 1) * body), :]
                remote(moved, moved, msend.at[j], mrecv.at[j], **mate(lax.rem(p + 1, h))).wait()

        return finish

    parts = psum.shape[0]
    rows_of = order // parts
    lump = rows_of // nr
    sends = [pair() for _ in range(4)]

    def band(n):
        return slice(n * rows_of, (n + 1) * rows_of)

    def share_of(n):
        for k in range(2):
            for q in range(h):
                ppack[n, q, k] = total[band(n), (k * h + q) * width:(k * h + q + 1) * width].astype(bf16)
        s, v = sends[0]
        return exchange(
            h, p, mate, lambda d: ppack.at[n, d], lambda k: pgot1.at[n, k], pgot1.at[n, pl.ds(0, h - 1)], s.at[n], v.at[n]
        )

    def crossing(n):
        s, v = sends[1]
        return remote(phalf.at[n, 0], phalf.at[n, 1], s.at[n], v.at[n], cols=other)

    def joined(n, k):
        mine_here = total[band(n), lanes(k * h + p, width)]
        for step in range(1, h):
            mine_here = mine_here + pgot1[n, lax.rem(p + step, h), k].astype(f32)
        return mine_here

    def launch(n):
        phalf[n, 0] = joined(n, 1 - y).astype(bf16)
        crossing(n).start()

    def spot(n, k):
        return psum.at[n, pl.ds(pl.multiple_of(k * lump, lump), lump), :]

    def scattered(n):
        crossing(n).wait()
        psum[n] = (joined(n, y) + phalf[n, 1].astype(f32)).astype(bf16)
        s, v = sends[2]
        done = exchange(
            nr, r, line, lambda d: spot(n, d), lambda k: pgot2.at[n, k], pgot2.at[n, pl.ds(0, nr - 1)], s.at[n], v.at[n]
        )
        pgot2[n, r] = psum[n, pl.ds(pl.multiple_of(r * lump, lump), lump), :]
        return done

    def gathered(n):
        def place_of(k):
            return pall.at[n, pl.ds(pl.multiple_of(k * lump, lump), lump), :]

        pall[n, pl.ds(pl.multiple_of(r * lump, lump), lump), :] = sum(
            (pgot2[n, k].astype(f32) for k in range(1, nr)), pgot2[n, 0].astype(f32)
        ).astype(bf16)
        s, v = sends[3]
        return exchange(nr, r, line, lambda d: place_of(r), lambda k: place_of(r), pgot2.at[n, pl.ds(0, nr - 1)], s.at[n], v.at[n])

    shared = [share_of(n) for n in range(parts // 2)]
    total[half:, :half] = inner(oext[1, size:bottom, :], zext[0])
    total[half:, half:] = inner(oext[1, size:bottom, :], zext[1])
    for n in range(parts // 2):
        shared[n]()
        launch(n)
    shared = [share_of(n) for n in range(parts // 2, parts)]
    for n in range(parts // 2, parts):
        shared[n - parts // 2]()
        launch(n)
    pl.when(y == 0)(lambda: send_late(late[1:]))
    finish_own = settle(1)

    @pl.when(y == 0)
    def _():
        for i in range(count):
            rows = slice(i * size, (i + 1) * size)
            home[rows, :] = dot(wsend[rows, :], rinv[:half, :half]).astype(bf16)

    spread_out = [scattered(n) for n in range(parts)]

    @pl.when(y == 1)
    def _():
        all_further(0).wait_recv()
        for i in (i for n in early for i in range(chunks[n][0], sum(chunks[n]))):
            rows = slice(i * size, (i + 1) * size)
            home[rows, :] = (dot(far[rows, :], rinv[:half, half:]) + dot(wsend[rows, :], rinv[half:, half:])).astype(bf16)

    brought = []
    for n in range(parts):
        spread_out[n]()
        brought.append(gathered(n))

    @pl.when(y == 1)
    def _():
        all_further(1).wait_recv()

    finish_other = settle(0)
    for n in range(parts):
        brought[n]()
        projected[band(n), :] = pall[n].astype(f32)

    finish_own()
    finish_other()

    @pl.when(y == 0)
    def _():
        all_further(0).wait_send()
        all_further(1).wait_send()

    for q in range(2):
        pl.when(flat < last)(lambda: halo(0, q).wait_send())
        pl.when(flat > 0)(lambda: halo(1, q).wait_send())
    remote(wsend, wsend, osem, orecv, cols=other).wait_send()
    over.wait_send()
    pl.when(r < nr - 1)(lambda: down().wait_send())
    pl.when(r > 0)(lambda: up().wait_send())
    for j in (0, 1):
        for s in range(4):
            each(j, s, lambda step: to_mate(j, s, step).wait_send())


def shards(nr, nc, basis, lower, diag, upper, inverse):
    blocks, size, _ = diag.shape
    width = basis.shape[1]
    h = nc // 2
    half = width * h
    order = 2 * half
    count = blocks // nc
    across = half // LANES
    body = count * size
    f32, bf16 = jnp.float32, jnp.bfloat16

    def parcel(lines, parts):
        piece = -(-lines // (h * parts * 8)) * 8
        return piece * parts, piece

    share, piece = parcel(across * (across + 1) // 2 * LANES, nr)
    xshare, xpiece = parcel(across * half, 2 * nr)
    parts = 4 if order // nr >= 8 * SUB else 1
    rows_of = order // parts
    dma = pltpu.SemaphoreType.DMA
    bext = (2, (count + 2) * size, half)
    ext = ((count + 2) * size, order)
    chunks = (count - 4) // 2 + 4
    square = pltpu.VMEM((half, half), f32)
    opflops = 16 * count * size * size * order + 6 * count * size * order * order
    return pl.pallas_call(
        functools.partial(whole_kernel, nr, nc),
        out_shape=(pltpu.VMEM(basis.shape, bf16), pltpu.VMEM((order, width), f32)),
        in_specs=[ANY] * 5,
        out_specs=(VMEM, VMEM),
        scratch_shapes=[
            pltpu.VMEM(bext, bf16), pltpu.VMEM(ext, bf16), pltpu.VMEM((body, half), bf16), pltpu.VMEM(bext, bf16),
            pltpu.VMEM((2, 4, count, size, size), bf16),
            square, square, pltpu.VMEM((order, order), f32), pltpu.VMEM((order, order), bf16),
            pltpu.VMEM((across, LANES, half), f32), pltpu.VMEM((LANES, LANES), f32), pltpu.VMEM((2, SUB, SUB, LANES), f32),
            square, square, square,
            pltpu.VMEM((h * share, LANES), f32), pltpu.VMEM((h, share, LANES), f32), pltpu.VMEM((share, LANES), f32),
            pltpu.VMEM((nr, piece, LANES), f32), pltpu.VMEM((2, h * share, LANES), f32),
            pltpu.VMEM((h * xshare, LANES), f32), pltpu.VMEM((h, xshare, LANES), f32), pltpu.VMEM((xshare, LANES), f32),
            pltpu.VMEM((2 * nr, xpiece, LANES), f32), pltpu.VMEM((h * xshare, LANES), f32),
            pltpu.VMEM((parts, h, 2, rows_of, width), bf16), pltpu.VMEM((parts, 2, rows_of, width), bf16),
            pltpu.VMEM((parts, nr, rows_of // nr, width), bf16), pltpu.VMEM((parts, rows_of, width), bf16),
            pltpu.VMEM((parts, h, 2, rows_of, width), bf16), pltpu.VMEM((parts, rows_of, width), bf16),
            pltpu.VMEM((body, half), bf16), pltpu.VMEM((body, half), bf16), pltpu.VMEM((2, body, half), bf16),
            pltpu.VMEM((2, body, half), bf16),
            pltpu.SemaphoreType.REGULAR((rounds(nr, nc) - 1,)),
            dma((2,)), dma((2, 4)), dma((2, 4)), dma((2,)),
            dma, dma, dma((2, 2)), dma((2, 2)), dma((2,)), dma((2,)),
            dma((2,)), dma((2,)), dma((2,)),
        ] + [dma] * 20 + [dma((parts,))] * 8,
        compiler_params=pltpu.CompilerParams(has_side_effects=True, collective_id=1),
        cost_estimate=pl.CostEstimate(flops=opflops, bytes_accessed=1 << 24, transcendentals=0),
        name="krylov",
    )(basis, lower, diag, upper, inverse)


def solution(mesh):
    in_specs = (
        P("rows", "cols"),
        P("rows", None, None),
        P("rows", None, None),
        P("rows", None, None),
        P("rows", None, None),
    )
    out_specs = (P("rows", "cols"), P(None, "cols"))
    body = functools.partial(shards, mesh.shape["rows"], mesh.shape["cols"])
    return jax.shard_map(body, mesh=mesh, in_specs=in_specs, out_specs=out_specs, check_vma=False)
```

```python
import functools

import jax
import jax.numpy as jnp
from jax import lax
from jax.experimental import pallas as pl
from jax.experimental.pallas import tpu as pltpu
from jax.sharding import PartitionSpec as P

LANES = 128
MESH = pl.DeviceIdType.MESH
VMEM = pl.BlockSpec(memory_space=pltpu.VMEM)
ANY = pl.BlockSpec(memory_space=pl.ANY)
SUB = 8
HI = lax.Precision.HIGHEST

def factor_tile(block, hold):
    size = block.shape[0]
    wide = (SUB, size)
    tiles = size // SUB
    row_of = lax.broadcasted_iota(jnp.int32, wide, 0)
    lane_of = lax.broadcasted_iota(jnp.int32, wide, 1)
    a = [block[t * SUB:(t + 1) * SUB, :] for t in range(tiles)]
    out = []
    for t in range(tiles):
        base = t * SUB
        at = a[t]
        last = t == tiles - 1
        inside = (lane_of >= base) & (lane_of < base + SUB)
        unity = jnp.where(lane_of == row_of + base, 1.0, 0.0).astype(jnp.float32)
        mixed = jnp.where(inside, unity, at)
        pivot = {}
        for j in range(SUB):
            hold[t % 2, j] = jnp.broadcast_to(at[:, base + j:base + j + 1], wide)
        for j in range(SUB):
            for i in range(j, SUB):
                pivot[i, j] = hold[t % 2, j, pl.ds(i, SUB, stride=0), :]
        rows = [jnp.broadcast_to(mixed[i:i + 1, :], wide) for i in range(SUB)]
        unit = {}
        solved = [None] * SUB
        if not last:
            ahead = jnp.where(inside, 0.0, a[t + 1])
            edge = [jnp.broadcast_to(a[t + 1][:, base + j:base + j + 1], wide) for j in range(SUB)]
        fin = jnp.zeros(wide, jnp.float32)
        for j in range(SUB):
            d = pivot[j, j]
            root = lax.rsqrt(d)
            inv = 1.0 / d
            for i in range(j + 1, SUB):
                unit[i, j] = pivot[i, j] * inv
            for i in range(j + 1, SUB):
                for q in range(j + 1, i + 1):
                    pivot[i, q] = pivot[i, q] - unit[i, j] * pivot[q, j]
            for i in range(j + 1, SUB):
                rows[i] = rows[i] - unit[i, j] * rows[j]
            fin = jnp.where(row_of == j, rows[j] * root, fin)
            if not last:
                solved[j] = rows[j] * inv
                ahead = ahead - edge[j] * solved[j]
                for q in range(j + 1, SUB):
                    edge[q] = edge[q] - edge[j] * unit[q, j]
        out.append(jnp.where(lane_of < base + SUB, fin, 0.0))
        if last:
            break
        a[t + 1] = ahead
        if t + 2 < tiles:
            for j in range(SUB - 1, -1, -1):
                for i in range(j):
                    solved[i] = solved[i] - unit[j, i] * solved[j]
        for s in range(t + 2, tiles):
            new = jnp.where(inside, 0.0, a[s])
            for j in range(SUB - 1, -1, -1):
                c = jnp.broadcast_to(a[s][:, base + j:base + j + 1], wide)
                new = new - c * solved[j]
            a[s] = new
    return jnp.concatenate(out, axis=0)


def eliminate(work_ref, b, out_ref, panel_ref, hold_ref):
    n, size, _ = work_ref.shape
    at = [work_ref[b, :, i * size:(i + 1) * size] for i in range(n)]
    block = at[0]
    for i in range(1, n):
        block = jnp.where(b == i, at[i], block)
    panel_ref[...] = factor_tile(block, hold_ref)

    def stage(k):
        linv = panel_ref[...]
        rows = slice(k * size, (k + 1) * size)
        if k:
            out_ref[rows, :k * size] = fine(linv, out_ref[rows, :k * size])
        out_ref[rows, rows] = linv
        if k + 1 < n:
            out_ref[rows, (k + 1) * size:] = jnp.zeros((size, (n - k - 1) * size), jnp.float32)
            right = fine(linv, work_ref[k, :, (k + 1) * size:n * size])
            known = jnp.concatenate([right, out_ref[rows, :(k + 1) * size]], axis=1)
            for i in range(k + 1, n):
                step = fine(right[:, (i - k - 1) * size:(i - k) * size], known, ((0,), (0,)))
                lines = slice(i * size, (i + 1) * size)
                cut = (n - k - 1) * size
                work_ref[i, :, (k + 1) * size:n * size] = work_ref[i, :, (k + 1) * size:n * size] - step[:, :cut]
                if k:
                    out_ref[lines, :k * size] = out_ref[lines, :k * size] - step[:, cut:cut + k * size]
                out_ref[lines, rows] = -step[:, cut + k * size:]

    for k in range(n):
        pl.when(b == k)(functools.partial(stage, k))


def dot(left, right):
    return jnp.dot(left, right, preferred_element_type=jnp.float32)


def inner(left, right):
    return lax.dot_general(
        left, right, (((0,), (0,)), ((), ())), preferred_element_type=jnp.float32
    )


def fine(left, right, dims=((1,), (0,))):
    return lax.dot_general(
        left, right, (dims, ((), ())), precision=HI, preferred_element_type=jnp.float32
    )


def remote(src, dst, send, recv, **where):
    return pltpu.make_async_remote_copy(
        src_ref=src, dst_ref=dst, send_sem=send, recv_sem=recv, device_id=where, device_id_type=MESH
    )


def exchange(count, me, where, source, target, whole, send, recv):
    for step in range(1, count):
        peer = lax.rem(me + step, count)
        remote(source(peer), target(me), send, recv, **where(peer)).start()

    def finish():
        if count > 1:
            remote(whole, whole, send, recv, **where(lax.rem(me + 1, count))).wait()

    return finish


def around(nr, nc, r, c):
    h = nc // 2
    for step in range(1, nc):
        yield True, r, lax.rem(c + step, nc)
    for by in (1, -1):
        there = (r + by >= 0) & (r + by < nr)
        for k in range(h):
            yield there, r + by, (c // h) * h + k
    for by in (2, -2):
        yield (r + by >= 0) & (r + by < nr), r + by, c


def rounds(nr, nc):
    h = nc // 2
    seen, edge, far = {(0, 0)}, {(0, 0)}, 0
    while len(seen) < nr * nc:
        new = set()
        for r, c in edge:
            new |= {(r, k) for k in range(nc)}
            new |= {(r + by, c // h * h + k) for by in (1, -1) for k in range(h)}
            new |= {(r + by, c) for by in (2, -2)}
        edge = {d for d in new if 0 <= d[0] < nr} - seen
        seen |= edge
        far += 1
    return far


def tell(sem, nr, nc, r, c):
    for there, row, col in around(nr, nc, r, c):
        def signal():
            pl.semaphore_signal(sem, inc=1, device_id=dict(rows=row, cols=col), device_id_type=MESH)

        if there is True:
            signal()
        else:
            pl.when(there)(signal)


def hear(sem, nr, nc, r, c):
    pl.semaphore_wait(sem, sum(1 if t is True else t.astype(jnp.int32) for t, _, _ in around(nr, nc, r, c)))


def lined(ref, start, extent):
    return ref.at[pl.ds(pl.multiple_of(start, 8), extent), :]


def summed(ref, count):
    return sum((ref[k] for k in range(1, count)), ref[0])


def whole_kernel(
    nr, nc, basis, lower, diag, upper, inverse, ortho, projected,
    bext, wext, wsend, oext, held, gy, gx, total, rinv, cwork, cpanel, hold, linv0, linv1, tall,
    ypack, ygot1, ypart, ygot2, yall, xpack, xgot1, xpart, xgot2, xall,
    pgot1, phalf, pgot2, psum, ppack, pall,
    far, home, zext, mix,
    known, wsem, bsend, brecv, esem, osem, orecv, hsend, hrecv, fsend, frecv, isem, msend, mrecv, *sems,
):
    sems = list(sems)

    def pair():
        return sems.pop(0), sems.pop(0)

    bf16, f32 = jnp.bfloat16, jnp.float32
    r, c = lax.axis_index("rows"), lax.axis_index("cols")
    h = nc // 2
    y, p = c // h, lax.rem(c, h)
    other = (1 - y) * h + p
    _, _, count, size, _ = held.shape
    width = basis.shape[1]
    half = width * h
    order = 2 * half
    body = count * size
    bottom = size + body
    team = 2 * nr
    seat = 2 * r + y

    def mate(k):
        return dict(cols=y * h + k)

    def member(k):
        return dict(rows=k // 2, cols=lax.rem(k, 2) * h + p)

    def line(k):
        return dict(rows=k)

    def at(i):
        return pl.ds(pl.multiple_of(i * size, size), size)

    def lanes(k, extent):
        return pl.ds(pl.multiple_of(k * extent, LANES), extent)

    wl, wd, wu, wi = (held.at[:, k] for k in range(4))
    for j, g in enumerate((other, c)):
        for k, part in enumerate((lower, diag, upper, inverse)):
            pltpu.make_async_copy(part.at[pl.ds(g * count, count)], held.at[j, k], wsem.at[j]).start()

    def weighed(j):
        pltpu.make_async_copy(held.at[1 - j], held.at[j], wsem.at[j]).wait()

    spans = [(0, size), (size, 3 * size), (bottom, size), (4 * size, body - 3 * size)]

    def group(j, k):
        return y * h + k if j else (1 - y) * h + k

    def leaving(j, s, k):
        start, extent = spans[s]
        return basis.at[pl.ds(pl.multiple_of(group(j, k) * body - size + start, size), extent), :]

    def landing(j, s, k):
        start, extent = spans[s]
        return bext.at[j, pl.ds(start, extent), lanes(k, width)]

    def within(s, g, action):
        if s == 0:
            pl.when(g > 0)(action)
        elif s == 2:
            pl.when(g < nc - 1)(action)
        else:
            action()

    def own(j, s):
        return pltpu.make_async_copy(leaving(j, s, p), landing(j, s, p), brecv.at[j, s])

    def to_mate(j, s, step):
        k = lax.rem(p + step, h)
        return remote(leaving(j, s, k), landing(j, s, p), bsend.at[j, s], brecv.at[j, s], **mate(k))

    def down():
        return remote(
            basis.at[pl.ds(nc * body - size, size), :], landing(1 - y, 0, p), esem.at[0],
            brecv.at[1 - y, 0], rows=r + 1, cols=y * h,
        )

    def up():
        return remote(
            basis.at[pl.ds(0, size), :], landing(y, 2, p), esem.at[1],
            brecv.at[y, 2], rows=r - 1, cols=y * h + h - 1,
        )

    for j in (0, 1):
        for s in (1, 3, 0, 2):
            within(s, group(j, p), lambda: own(j, s).start())

    barrier = pltpu.get_barrier_semaphore()
    tell(barrier, nr, nc, r, c)
    hear(barrier, nr, nc, r, c)
    heard = known.shape[0]
    tell(known.at[0], nr, nc, r, c)
    told = [0]

    def spread():
        if told[0] < heard:
            hear(known.at[told[0]], nr, nc, r, c)
            told[0] += 1
            if told[0] < heard:
                tell(known.at[told[0]], nr, nc, r, c)

    def each(j, s, action):
        for step in range(1, h):
            k = lax.rem(p + step, h)
            within(s, group(j, k), functools.partial(action, step))

    for s in (1, 3):
        for step in range(1, h):
            to_mate(0, s, step).start()
    pl.when(r < nr - 1)(lambda: down().start())
    pl.when(r > 0)(lambda: up().start())
    for j, s in ((0, 0), (0, 2), (1, 1), (1, 3), (1, 0), (1, 2)):
        each(j, s, lambda step: to_mate(j, s, step).start())

    for j in (0, 1):
        @pl.when((r == 0) & (group(j, p) == 0))
        def _():
            bext[j, 0:size, :] = jnp.zeros((size, half), bf16)

        @pl.when((r == nr - 1) & (group(j, p) == nc - 1))
        def _():
            bext[j, bottom:bottom + size, :] = jnp.zeros((size, half), bf16)

    @pl.when((r == 0) & (c == 0))
    def _():
        wext[0:size, :] = jnp.zeros((size, order), bf16)

    @pl.when((r == nr - 1) & (c == nc - 1))
    def _():
        wext[bottom:bottom + size, :] = jnp.zeros((size, order), bf16)

    def arrive(j, s):
        g = group(j, p)
        start, extent = spans[s]
        full = bext.at[j, pl.ds(start, extent), :]
        comes = {0: (g > 0) | (r > 0), 2: (g < nc - 1) | (r < nr - 1)}.get(s, r >= 0)
        pl.when(comes)(lambda: pltpu.make_async_copy(bext.at[1 - j, pl.ds(start, extent), :], full, brecv.at[j, s]).wait())

    def applied(field, j, some, columns, out):
        for i in some:
            mixed = (
                dot(wl[j, i], field[i * size:(i + 1) * size, columns])
                + dot(wd[j, i], field[(i + 1) * size:(i + 2) * size, columns])
                + dot(wu[j, i], field[(i + 2) * size:(i + 3) * size, columns])
            )
            mix[j, i * size:(i + 1) * size, :] = mixed.astype(bf16)
        for i in some:
            out(i, dot(wi[j, i], mix[j, i * size:(i + 1) * size, :]).astype(bf16))

    mine = lanes(y, half)
    chunks = [(1, 1), (2, 1)] + [(i, 2) for i in range(3, count - 1, 2)] + [(0, 1), (count - 1, 1)]

    def cross(n, to=None):
        start, extent = chunks[n][0] * size, chunks[n][1] * size
        return remote(
            wsend.at[pl.ds(start, extent), :],
            wext.at[pl.ds(size + start, extent), mine if to is None else to],
            osem, orecv, cols=other,
        )

    weighed(0)
    arrive(0, 1)

    def first(some):
        def keep(i, w):
            wsend[i * size:(i + 1) * size, :] = w

        applied(bext.at[0], 0, some, slice(None), keep)

    def second(some):
        def keep(i, w):
            wext[(i + 1) * size:(i + 2) * size, mine] = w

        applied(bext.at[1], 1, some, slice(None), keep)

    for n in range(len(chunks) - 2):
        start, extent = chunks[n]
        if n == 1:
            arrive(0, 3)
        first(range(start, start + extent))
        cross(n).start()
        if n == 1:
            spread()
    weighed(1)
    arrive(1, 1)
    arrive(1, 3)
    second(range(1, count - 1))
    spread()
    mid = slice(size, body - size)
    gy[...] = inner(wsend[mid, :], wsend[mid, :])
    spread()
    own_half = wext[2 * size:body, mine]
    gy[...] += inner(own_half, own_half)
    arrive(0, 0)
    arrive(0, 2)
    first((0, count - 1))
    for n in range(len(chunks) - 2, len(chunks)):
        cross(n).start()
    spread()
    arrive(1, 0)
    arrive(1, 2)
    second((0, count - 1))
    for _ in range(heard):
        spread()
    for rows in (slice(0, size), slice(body - size, body)):
        own_half = wext[rows.start + size:rows.stop + size, mine]
        gy[...] += inner(wsend[rows, :], wsend[rows, :]) + inner(own_half, own_half)

    early = list(range(len(chunks) // 2))
    late = sorted(range(len(chunks) // 2, len(chunks)), key=lambda n: chunks[n][1])

    def further(n):
        start, extent = chunks[n][0] * size, chunks[n][1] * size
        if n in early:
            source, target = wext.at[pl.ds(size + start, extent), :half], far.at[pl.ds(start, extent), :]
        else:
            source, target = oext.at[1, pl.ds(size + start, extent), :], home.at[pl.ds(start, extent), :]
        return remote(source, target, fsend.at[int(n in late)], frecv.at[int(n in late)], cols=other)

    def all_further(kind):
        some = (early, late)[kind]
        extent = sum(chunks[n][1] for n in some) * size
        part = far.at[pl.ds(0, extent), :]
        return remote(part, part, fsend.at[kind], frecv.at[kind], cols=other)

    def send_late(some):
        for n in some:
            further(n).start()

    across = half // LANES
    place = 0
    for i in range(across):
        for j in range(i, across):
            ypack[place * LANES:(place + 1) * LANES, :] = gy[
                i * LANES:(i + 1) * LANES, j * LANES:(j + 1) * LANES
            ]
            place += 1
    if ypack.shape[0] > place * LANES:
        ypack[place * LANES:, :] = jnp.zeros((ypack.shape[0] - place * LANES, LANES), f32)
    share, piece = ygot1.shape[1], ygot2.shape[1]
    s, v = pair()
    finish = exchange(
        h, p, mate, lambda d: lined(ypack, d * share, share), lambda k: ygot1.at[k],
        ygot1.at[pl.ds(0, h - 1)], s, v
    )
    ygot1[p] = ypack[pl.ds(pl.multiple_of(p * share, 8), share), :]
    finish()
    ypart[...] = summed(ygot1, h)
    s, v = pair()
    finish = exchange(
        nr, r, line, lambda d: lined(ypart, d * piece, piece), lambda k: ygot2.at[k],
        ygot2.at[pl.ds(0, nr - 1)], s, v
    )
    ygot2[r] = ypart[pl.ds(pl.multiple_of(r * piece, 8), piece), :]
    finish()

    def yspot(k):
        return yall.at[y, pl.ds(pl.multiple_of(p * share + k * piece, 8), piece), :]

    def yshare(side, k):
        return yall.at[side, pl.ds(pl.multiple_of(k * share, 8), share), :]

    yall[y, pl.ds(pl.multiple_of(p * share + r * piece, 8), piece), :] = summed(ygot2, nr)
    s, v = pair()
    exchange(nr, r, line, lambda d: yspot(r), lambda k: yspot(r), ygot2.at[pl.ds(0, nr - 1)], s, v)()
    s, v = pair()
    over = remote(yshare(y, p), yshare(y, p), s, v, cols=other)
    over.start()

    def both(side, sems_of):
        rest = yall.at[side, pl.ds(0, (h - 1) * share), :]
        exchange(h, p, mate, lambda d: yshare(side, p), lambda k: yshare(side, p), rest, *sems_of)()

    both(y, pair())
    opposite_sems = pair()

    def opposite():
        over.wait_recv()
        both(1 - y, opposite_sems)

    def load(which):
        place = 0
        for i in range(across):
            for j in range(i, across):
                cwork[i, :, j * LANES:(j + 1) * LANES] = yall[which, place * LANES:(place + 1) * LANES, :]
                place += 1

    flat = r * nc + c
    last = nr * nc - 1

    def halo(kind, q):
        start = (body, size)[kind]
        target = (0, bottom)[kind]
        to = flat + (1, -1)[kind]
        part = pl.ds(q * half, half)
        return remote(
            wext.at[pl.ds(start, size), part], wext.at[pl.ds(target, size), part], hsend.at[kind, q],
            hrecv.at[kind, q], rows=to // nc, cols=lax.rem(to, nc),
        )


    theirs = lanes(1 - y, half)
    xshare, xpiece = xgot1.shape[1], xgot2.shape[1]
    def xspot(k):
        return lined(xall, p * xshare + k * xpiece, xpiece)
    def xsection(k):
        return lined(xall, k * xshare, xshare)
    xcore, xscatter, xgather, xcopy = pair(), pair(), pair(), pair()

    def scatter():
        return exchange(
            team, seat, member, lambda d: lined(xpart, d * xpiece, xpiece), lambda k: xgot2.at[k],
            xgot2.at[pl.ds(0, team - 1)], *xscatter,
        )

    def turned(columns):
        depth = columns.stop
        oext[columns.start // half, size:bottom, :] = dot(wext[size:bottom, :depth], rinv[:depth, columns]).astype(bf16)

    def imaged(q):
        def keep(i, z):
            zext[q, i * size:(i + 1) * size, :] = z

        applied(oext.at[q], 1, range(count), slice(None), keep)

    def cross_half():
        crossed = wext.at[pl.ds(size, body), theirs]
        remote(crossed, crossed, osem, orecv, cols=other).wait_recv()
        gx[...] = inner(wext[size:bottom, :half], wext[size:bottom, half:])
        for j in range(across):
            xpack[j * half:(j + 1) * half, :] = gx[:, j * LANES:(j + 1) * LANES]
        if xpack.shape[0] > across * half:
            xpack[across * half:, :] = jnp.zeros((xpack.shape[0] - across * half, LANES), f32)
        finish = exchange(
            h, p, mate, lambda d: lined(xpack, d * xshare, xshare), lambda k: xgot1.at[k],
            xgot1.at[pl.ds(0, h - 1)], *xcore
        )
        xgot1[p] = xpack[pl.ds(pl.multiple_of(p * xshare, 8), xshare), :]
        finish()
        xpart[...] = summed(xgot1, h)
        scatter()
        pl.when(flat < last)(lambda: halo(0, 0).start())
        pl.when(flat > 0)(lambda: halo(1, 0).start())

    def join():
        arrived = xgot2.at[pl.ds(0, team - 1)]
        remote(arrived, arrived, *xscatter, **member(lax.rem(seat + 1, team))).wait()
        xgot2[seat] = xpart[pl.ds(pl.multiple_of(seat * xpiece, 8), xpiece), :]
        xall[pl.ds(pl.multiple_of(p * xshare + seat * xpiece, 8), xpiece), :] = summed(xgot2, team)
        exchange(team, seat, member, lambda d: xspot(seat), lambda k: xspot(seat), arrived, *xgather)
        pl.when(flat < last)(lambda: halo(0, 1).start())
        pl.when(flat > 0)(lambda: halo(1, 1).start())

        @pl.when(y == 0)
        def _():
            for n in early:
                further(n).start()

    def rest():
        linv0[...] = linv1[...]
        rinv[:half, :half] = linv0[...].T.astype(bf16)
        turned(slice(0, half))

        def early_image():
            pl.when(flat > 0)(lambda: halo(0, 0).wait_recv())
            pl.when(flat < last)(lambda: halo(1, 0).wait_recv())
            oext[0, :size, :] = dot(wext[:size, :half], rinv[:half, :half]).astype(bf16)
            oext[0, bottom:, :] = dot(wext[bottom:, :half], rinv[:half, :half]).astype(bf16)
            imaged(0)
            total[:half, :half] = inner(oext[0, size:bottom, :], zext[0])

        pl.when(y == 0)(early_image)
        pl.when(y == 0)(opposite)
        arrived = xgot2.at[pl.ds(0, team - 1)]
        remote(arrived, arrived, *xgather, **member(lax.rem(seat + 1, team))).wait()
        finish = exchange(
            h, p, mate, lambda d: xsection(p), lambda k: xsection(p), lined(xall, 0, (h - 1) * xshare), *xcopy
        )
        pl.when(y == 1)(early_image)
        finish()
        for j in range(across):
            gx[:, j * LANES:(j + 1) * LANES] = xall[j * half:(j + 1) * half, :]
        tall[...] = fine(linv0[...], gx[...])
        load(1)
        for i in range(across):
            cwork[i, :, i * LANES:] = cwork[i, :, i * LANES:] - fine(
                tall[:, i * LANES:(i + 1) * LANES], tall[:, i * LANES:], ((0,), (0,))
            )
        gx[...] = fine(tall[...], linv0[...], ((0,), (0,)))

    pl.when(y == 0)(lambda: load(0))

    def factor_step(g, carry):
        @pl.when((g == 0) & (y == 1))
        def _():
            cross_half()
            opposite()
            load(0)

        eliminate(cwork, lax.rem(g, across), linv1, cpanel, hold)
        pl.when((g == 0) & (y == 0))(cross_half)
        pl.when(((g == 0) & (y == 1)) | ((g == across - 1) & (y == 0)))(join)
        pl.when(g == across - 1)(rest)
        return carry

    lax.fori_loop(0, 2 * across, factor_step, 0)
    rinv[half:, half:] = linv1[...].T.astype(bf16)
    rinv[:half, half:] = (-fine(gx[...], linv1[...], ((0,), (1,)))).astype(bf16)
    pl.when(flat > 0)(lambda: halo(0, 1).wait_recv())
    pl.when(flat < last)(lambda: halo(1, 1).wait_recv())
    oext[1] = dot(wext[...], rinv[:, half:]).astype(bf16)
    pl.when(y == 0)(lambda: send_late(late[:1]))
    imaged(1)
    total[:half, half:] = inner(oext[0, size:bottom, :], zext[1])
    def place(j, source, first, k):
        return source.at[pl.ds(first, body), k], ortho.at[pl.ds(pl.multiple_of((c if j else other) * body, size), body), :]

    def settle(j):
        source, first = (oext.at[y], size) if j else (home, 0)

        def col(k):
            return lanes(k, width)

        own_copy = pltpu.make_async_copy(*place(j, source, first, col(p)), isem.at[j])
        own_copy.start()
        for step in range(1, h):
            k = lax.rem(p + step, h)
            src_ref, dst_ref = place(j, source, first, col(k))
            remote(src_ref, dst_ref, msend.at[j], mrecv.at[j], **mate(k)).start()

        def finish():
            own_copy.wait()
            if h > 1:
                moved = ortho.at[pl.ds(0, (h - 1) * body), :]
                remote(moved, moved, msend.at[j], mrecv.at[j], **mate(lax.rem(p + 1, h))).wait()

        return finish

    parts = psum.shape[0]
    rows_of = order // parts
    lump = rows_of // nr
    sends = [pair() for _ in range(4)]

    def band(n):
        return slice(n * rows_of, (n + 1) * rows_of)

    def share_of(n):
        for k in range(2):
            for q in range(h):
                ppack[n, q, k] = total[band(n), (k * h + q) * width:(k * h + q + 1) * width].astype(bf16)
        s, v = sends[0]
        return exchange(
            h, p, mate, lambda d: ppack.at[n, d], lambda k: pgot1.at[n, k], pgot1.at[n, pl.ds(0, h - 1)], s.at[n], v.at[n]
        )

    def crossing(n):
        s, v = sends[1]
        return remote(phalf.at[n, 0], phalf.at[n, 1], s.at[n], v.at[n], cols=other)

    def joined(n, k):
        mine_here = total[band(n), lanes(k * h + p, width)]
        for step in range(1, h):
            mine_here = mine_here + pgot1[n, lax.rem(p + step, h), k].astype(f32)
        return mine_here

    def launch(n):
        phalf[n, 0] = joined(n, 1 - y).astype(bf16)
        crossing(n).start()

    def spot(n, k):
        return psum.at[n, pl.ds(pl.multiple_of(k * lump, lump), lump), :]

    def scattered(n):
        crossing(n).wait()
        psum[n] = (joined(n, y) + phalf[n, 1].astype(f32)).astype(bf16)
        s, v = sends[2]
        done = exchange(
            nr, r, line, lambda d: spot(n, d), lambda k: pgot2.at[n, k], pgot2.at[n, pl.ds(0, nr - 1)], s.at[n], v.at[n]
        )
        pgot2[n, r] = psum[n, pl.ds(pl.multiple_of(r * lump, lump), lump), :]
        return done

    def gathered(n):
        def place_of(k):
            return pall.at[n, pl.ds(pl.multiple_of(k * lump, lump), lump), :]

        pall[n, pl.ds(pl.multiple_of(r * lump, lump), lump), :] = sum(
            (pgot2[n, k].astype(f32) for k in range(1, nr)), pgot2[n, 0].astype(f32)
        ).astype(bf16)
        s, v = sends[3]
        return exchange(nr, r, line, lambda d: place_of(r), lambda k: place_of(r), pgot2.at[n, pl.ds(0, nr - 1)], s.at[n], v.at[n])

    shared = [share_of(n) for n in range(parts // 2)]
    total[half:, :half] = inner(oext[1, size:bottom, :], zext[0])
    total[half:, half:] = inner(oext[1, size:bottom, :], zext[1])
    for n in range(parts // 2):
        shared[n]()
        launch(n)
    shared = [share_of(n) for n in range(parts // 2, parts)]
    for n in range(parts // 2, parts):
        shared[n - parts // 2]()
        launch(n)
    pl.when(y == 0)(lambda: send_late(late[1:]))
    finish_own = settle(1)

    @pl.when(y == 0)
    def _():
        for i in range(count):
            rows = slice(i * size, (i + 1) * size)
            home[rows, :] = dot(wsend[rows, :], rinv[:half, :half]).astype(bf16)

    spread_out = [scattered(n) for n in range(parts)]

    @pl.when(y == 1)
    def _():
        all_further(0).wait_recv()
        for i in (i for n in early for i in range(chunks[n][0], sum(chunks[n]))):
            rows = slice(i * size, (i + 1) * size)
            home[rows, :] = (dot(far[rows, :], rinv[:half, half:]) + dot(wsend[rows, :], rinv[half:, half:])).astype(bf16)

    brought = []
    for n in range(parts):
        spread_out[n]()
        brought.append(gathered(n))

    @pl.when(y == 1)
    def _():
        all_further(1).wait_recv()

    finish_other = settle(0)
    for n in range(parts):
        brought[n]()
        projected[band(n), :] = pall[n].astype(f32)

    finish_own()
    finish_other()

    @pl.when(y == 0)
    def _():
        all_further(0).wait_send()
        all_further(1).wait_send()

    for q in range(2):
        pl.when(flat < last)(lambda: halo(0, q).wait_send())
        pl.when(flat > 0)(lambda: halo(1, q).wait_send())
    remote(wsend, wsend, osem, orecv, cols=other).wait_send()
    over.wait_send()
    pl.when(r < nr - 1)(lambda: down().wait_send())
    pl.when(r > 0)(lambda: up().wait_send())
    for j in (0, 1):
        for s in range(4):
            each(j, s, lambda step: to_mate(j, s, step).wait_send())


def shards(nr, nc, basis, lower, diag, upper, inverse):
    blocks, size, _ = diag.shape
    width = basis.shape[1]
    h = nc // 2
    half = width * h
    order = 2 * half
    count = blocks // nc
    across = half // LANES
    body = count * size
    f32, bf16 = jnp.float32, jnp.bfloat16

    def parcel(lines, parts):
        piece = -(-lines // (h * parts * 8)) * 8
        return piece * parts, piece

    share, piece = parcel(across * (across + 1) // 2 * LANES, nr)
    xshare, xpiece = parcel(across * half, 2 * nr)
    parts = 4 if order // nr >= 8 * SUB else 1
    rows_of = order // parts
    dma = pltpu.SemaphoreType.DMA
    bext = (2, (count + 2) * size, half)
    ext = ((count + 2) * size, order)
    chunks = (count - 4) // 2 + 4
    square = pltpu.VMEM((half, half), f32)
    opflops = 16 * count * size * size * order + 6 * count * size * order * order
    return pl.pallas_call(
        functools.partial(whole_kernel, nr, nc),
        out_shape=(pltpu.VMEM(basis.shape, bf16), pltpu.VMEM((order, width), f32)),
        in_specs=[ANY] * 5,
        out_specs=(VMEM, VMEM),
        scratch_shapes=[
            pltpu.VMEM(bext, bf16), pltpu.VMEM(ext, bf16), pltpu.VMEM((body, half), bf16), pltpu.VMEM(bext, bf16),
            pltpu.VMEM((2, 4, count, size, size), bf16),
            square, square, pltpu.VMEM((order, order), f32), pltpu.VMEM((order, order), bf16),
            pltpu.VMEM((across, LANES, half), f32), pltpu.VMEM((LANES, LANES), f32), pltpu.VMEM((2, SUB, SUB, LANES), f32),
            square, square, square,
            pltpu.VMEM((h * share, LANES), f32), pltpu.VMEM((h, share, LANES), f32), pltpu.VMEM((share, LANES), f32),
            pltpu.VMEM((nr, piece, LANES), f32), pltpu.VMEM((2, h * share, LANES), f32),
            pltpu.VMEM((h * xshare, LANES), f32), pltpu.VMEM((h, xshare, LANES), f32), pltpu.VMEM((xshare, LANES), f32),
            pltpu.VMEM((2 * nr, xpiece, LANES), f32), pltpu.VMEM((h * xshare, LANES), f32),
            pltpu.VMEM((parts, h, 2, rows_of, width), bf16), pltpu.VMEM((parts, 2, rows_of, width), bf16),
            pltpu.VMEM((parts, nr, rows_of // nr, width), bf16), pltpu.VMEM((parts, rows_of, width), bf16),
            pltpu.VMEM((parts, h, 2, rows_of, width), bf16), pltpu.VMEM((parts, rows_of, width), bf16),
            pltpu.VMEM((body, half), bf16), pltpu.VMEM((body, half), bf16), pltpu.VMEM((2, body, half), bf16),
            pltpu.VMEM((2, body, half), bf16),
            pltpu.SemaphoreType.REGULAR((rounds(nr, nc) - 1,)),
            dma((2,)), dma((2, 4)), dma((2, 4)), dma((2,)),
            dma, dma, dma((2, 2)), dma((2, 2)), dma((2,)), dma((2,)),
            dma((2,)), dma((2,)), dma((2,)),
        ] + [dma] * 20 + [dma((parts,))] * 8,
        compiler_params=pltpu.CompilerParams(has_side_effects=True, collective_id=1),
        cost_estimate=pl.CostEstimate(flops=opflops, bytes_accessed=1 << 24, transcendentals=0),
        name="krylov",
    )(basis, lower, diag, upper, inverse)


def solution(mesh):
    in_specs = (
        P("rows", "cols"),
        P("rows", None, None),
        P("rows", None, None),
        P("rows", None, None),
        P("rows", None, None),
    )
    out_specs = (P("rows", "cols"), P(None, "cols"))
    body = functools.partial(shards, mesh.shape["rows"], mesh.shape["cols"])
    return jax.shard_map(body, mesh=mesh, in_specs=in_specs, out_specs=out_specs, check_vma=False)
```
